128 devices in a mesh: dim: 16 (over y, x), batch: 8 (over z, core).
Axes of the slice: x: 4, y: 4, z: 4, core: 2. Of those that a mesh axis runs over, the one named last changes fastest.
Arguments:
- start: float32 [2048, 4096], P('batch', 'dim'), may hold values from -6 to 6
- increments: float32 [3, 2048, 4096], P(None, 'batch', 'dim'), may hold values from -0.75 to 0.75
- w_in: bfloat16 [4096, 4096], P(None, 'dim'), may hold values from -0.09375 to 0.09375
- w_out: bfloat16 [4096, 4096], P('dim'), may hold values from -0.09375 to 0.09375
- initial: float32 [], replicated, may hold values from 4 to 5.5
Outputs:
- residual: float32 [2048], P('batch')
- grad_in: float32 [4096, 4096], P('batch', 'dim')
- grad_out: float32 [4096, 4096], P('dim', 'batch')
The draws below stay inside these ranges and needn't reach their ends.
All inputs are finite; a program needn't handle non-finite values.
Results may differ from the reference program's by a relative error of at most 0.0051.
Values may be sent and summed in bfloat16 or wider, within the bound.
A program may use at most 128 MiB of HBM per device.

```python
import math
import jax
import jax.numpy as jnp
from jax import lax

D = 4096
H = 4096
STEPS = 3
PATHS = 2048


def block_levels(stream_key, shape, cuts, low, top_value):
    def one(axis_at, blocks):
        steps = jax.random.uniform(jax.random.fold_in(jax.random.fold_in(stream_key, 6), axis_at), (blocks,), jnp.float32, low / len(cuts), top_value / len(cuts))
        return jnp.repeat(jnp.exp(steps), shape[axis_at] // blocks).reshape((-1,) + (1,) * (len(shape) - axis_at - 1))

    loudness = one(*cuts[0])
    for cut in cuts[1:]:
        loudness = loudness * one(*cut)
    return loudness


def noise(rng, extent, deviation, bound, cuts=(), kind=jnp.bfloat16):
    values = jax.random.normal(rng, extent, jnp.float32) * deviation
    if len(cuts) > 0:
        values = block_levels(rng, extent, cuts, -0.22, 0.18) * values
    return jnp.clip(values, min=-bound, max=bound).astype(kind)


def setup_inputs(seed: int = 0) -> dict:
    key_of = jax.random.split(jax.random.key(seed), 6)
    return {
        "start": noise(key_of[0], (PATHS, D), 1.0, 6.0, ((0, 8), (1, 16)), jnp.float32),
        "increments": noise(key_of[1], (STEPS, PATHS, D), 0.125, 0.75, ((1, 8), (2, 16)), jnp.float32),
        "w_in": noise(key_of[2], (D, H), D ** -0.5, 0.09375, ((1, 16),)),
        "w_out": noise(key_of[3], (H, D), H ** -0.5, 0.09375, ((0, 16),)),
        "initial": jnp.clip(jax.random.uniform(key_of[4], (), jnp.float32, 4.0, 5.5), 4.0, 5.5),
    }


time_step = 1.0 / 64.0
lam_coef = 50.0
noise_coef = math.sqrt(2.0)

def reference(start, increments, w_in, w_out, initial):
    zscale = 2.0 / math.sqrt(D)
    state = start
    saved = []
    ysum = jnp.zeros((start.shape[0],), jnp.float32)
    for step in range(STEPS):
        inc = increments[step]
        xb = state.astype(jnp.bfloat16)
        hidden = jnp.dot(xb, w_in, preferred_element_type=jnp.float32)
        act = jax.nn.silu(hidden).astype(jnp.bfloat16)
        zval = zscale * jnp.dot(act, w_out, preferred_element_type=jnp.float32)
        ysum = ysum + 0.5 * lam_coef * time_step * lax.optimization_barrier(jnp.sum(zval * zval, 1)) + lax.optimization_barrier(jnp.sum(zval * inc, 1))
        saved.append((xb, hidden, act, zval))
        state = state + noise_coef * inc
    norm_sq = lax.optimization_barrier(jnp.sum(state * state, 1))
    residual = initial + ysum - jnp.log((1.0 + norm_sq) * 0.5)
    grad_in = jnp.zeros(w_in.shape, jnp.float32)
    grad_out = jnp.zeros(w_out.shape, jnp.float32)
    for step in range(STEPS):
        xb, hidden, act, zval = saved[step]
        gz = (zscale * residual[:, None] * (lam_coef * time_step * zval + increments[step])).astype(jnp.bfloat16)
        grad_out = grad_out + jnp.dot(act.T, gz, preferred_element_type=jnp.float32)
        ga = jnp.dot(gz, w_out.T, preferred_element_type=jnp.float32)
        sig = jax.nn.sigmoid(hidden)
        gh = (ga * sig * (1.0 + hidden * (1.0 - sig))).astype(jnp.bfloat16)
        grad_in = grad_in + jnp.dot(xb.T, gh, preferred_element_type=jnp.float32)
    return (residual, grad_in, grad_out)
```

```python
import math

import jax
import jax.numpy as jnp
from jax import lax
from jax.sharding import Mesh
from jax.sharding import PartitionSpec as P

D = 4096
STEPS = 3
DIM = ("y", "x")
BATCH = ("z", "c")

time_step = 1.0 / 64.0
lam_coef = 50.0
noise_coef = math.sqrt(2.0)


def a2a(array, axis):
    return lax.all_to_all(array, axis, split_axis=0, concat_axis=0, tiled=True)


def scatter_sum(parts, axis):
    got = a2a(parts.astype(jnp.bfloat16), axis)
    return jnp.sum(got.astype(jnp.float32), 0)


def on_device(start, increments, w_in, w_out, initial):
    zscale = 2.0 / math.sqrt(D)
    rows, width = start.shape
    f32, bf16 = jnp.float32, jnp.bfloat16
    win = a2a(w_in.reshape(4, 4, width, width).transpose(1, 0, 2, 3), "x")
    wout = a2a(w_out.reshape(width, 4, 4, width).transpose(2, 1, 0, 3), "x")
    states = [start]
    for step in range(STEPS):
        states.append(states[-1] + noise_coef * increments[step])
    xb = jnp.stack(states[:STEPS]).astype(bf16).reshape(STEPS * rows, width)
    inc = increments.reshape(STEPS * rows, width)
    xg = lax.all_gather(xb, "y")
    h = scatter_sum(jnp.einsum("jrd,ijdh->irh", xg, win, preferred_element_type=f32), "x")
    act = jax.nn.silu(h).astype(bf16)
    ag = lax.all_gather(act, "x")
    z = zscale * scatter_sum(jnp.einsum("irh,ijhd->jrd", ag, wout, preferred_element_type=f32), "y")
    terms = jnp.sum((0.5 * lam_coef * time_step * z * z + z * inc).reshape(STEPS, rows, width), (0, 2))
    norm = jnp.sum(states[STEPS] * states[STEPS], 1)
    both = lax.psum(jnp.stack([terms, norm]), DIM)
    residual = initial + both[0] - jnp.log((1.0 + both[1]) * 0.5)
    scale = jnp.tile(zscale * residual, STEPS)[:, None]
    gz = (scale * (lam_coef * time_step * z + inc)).astype(bf16)
    gg = lax.all_gather(gz, "y")
    ga = scatter_sum(jnp.einsum("jrd,ijhd->irh", gg, wout, preferred_element_type=f32), "x")
    sig = jax.nn.sigmoid(h)
    gh = (ga * sig * (1.0 + h * (1.0 - sig))).astype(bf16)
    hg = lax.all_gather(gh, "x")
    gout = jnp.einsum("irh,jrd->jihd", ag, gg, preferred_element_type=f32)
    gin = jnp.einsum("jrd,irh->jidh", xg, hg, preferred_element_type=f32)
    grads = jnp.stack([gin, gout], 1)
    grads = grads.reshape(4, 2, 2, 2, width, width).transpose(3, 0, 1, 2, 4, 5)
    grads = lax.psum_scatter(grads.reshape(2, 4, -1), "c", scatter_dimension=0, tiled=False)
    grads = scatter_sum(grads, "z").reshape(2, 2, width, width)
    grads = lax.all_gather(grads, "c")
    grads = grads.transpose(2, 0, 1, 3, 4).reshape(4, -1)
    grads = a2a(grads.astype(bf16), "x").astype(f32).reshape(2, 2, 2, width, width)
    mine = lax.dynamic_index_in_dim(grads, lax.axis_index("c"), 0, keepdims=False)
    return residual, mine[:, 0].reshape(2 * width, width), mine[:, 1].transpose(1, 0, 2).reshape(width, 2 * width)


def solution(mesh):
    finer = Mesh(mesh.devices.reshape(4, 4, 4, 2), ("y", "x", "z", "c"))
    return jax.shard_map(
        on_device,
        mesh=finer,
        in_specs=(P(BATCH, DIM), P(None, BATCH, DIM), P(None, DIM), P(DIM, None), P()),
        out_specs=(P(BATCH), P(BATCH, DIM), P(DIM, BATCH)),
        check_vma=False,
    )
```

```python
import math

import jax
import jax.numpy as jnp
from jax import lax
from jax.experimental import pallas as pl
from jax.experimental.pallas import tpu as pltpu
from jax.sharding import Mesh
from jax.sharding import PartitionSpec as P

D = 4096
STEPS = 3
B = 256
H = B // 2
DIM = ("y", "x")
BATCH = ("z", "c")
MESH = pl.DeviceIdType.MESH
f32, bf16 = jnp.float32, jnp.bfloat16

time_step = 1.0 / 64.0
lam_coef = 50.0
noise_coef = math.sqrt(2.0)
zscale = 2.0 / math.sqrt(D)
COPIES = 240


def place(pos, extent):
    return pl.ds(pl.multiple_of(pos * extent, extent), extent)


class Net:
    def __init__(self, send, recv):
        self.send, self.recv, self.count, self.begun = send, recv, 0, []

    def copy(self, src, dst, device):
        k = self.count
        self.count += 1
        assert self.count <= COPIES
        return pltpu.make_async_remote_copy(
            src_ref=src,
            dst_ref=dst,
            send_sem=self.send.at[k],
            recv_sem=self.recv.at[k],
            device_id=device,
            device_id_type=MESH,
        )

    def start(self, copy):
        copy.start()
        self.begun.append(copy)

    def drain(self):
        for copy in self.begun:
            copy.wait_send()


class Gather:
    def __init__(self, net, axis, view):
        p = lax.axis_index(axis)
        r, l = lax.rem(p + 1, 4), lax.rem(p + 3, 4)
        self.net = net
        self.copies = [
            net.copy(view(owner, half), view(owner, half), {axis: to})
            for owner, half, to in ((p, 0, r), (p, 1, l), (p, 1, r), (p, 0, l), (l, 0, r), (r, 1, l))
        ]

    def start(self):
        for k in range(4):
            self.net.start(self.copies[k])

    def mid(self):
        for k in range(2):
            self.copies[k].wait_recv()
            self.net.start(self.copies[4 + k])

    def finish(self):
        for k in range(2, 6):
            self.copies[k].wait_recv()


class Scatter:
    def __init__(self, net, axis, sent, far, near, held):
        p = lax.axis_index(axis)
        r, l = {axis: lax.rem(p + 1, 4)}, {axis: lax.rem(p + 3, 4)}
        self.net, self.sent, self.far, self.near, self.held = net, sent, far, near, held
        self.copies = {
            (2, 0): net.copy(sent.at[1, 0], far.at[0], r),
            (2, 1): net.copy(sent.at[1, 1], far.at[1], l),
            (1, 1): net.copy(sent.at[0, 1], near.at[0, 1], r),
            (3, 0): net.copy(sent.at[2, 0], near.at[1, 0], l),
            (1, 0): net.copy(sent.at[0, 0], near.at[0, 0], r),
            (3, 1): net.copy(sent.at[2, 1], near.at[1, 1], l),
        }

    def put(self, k, half, value):
        if (k, half) in ((2, 0), (2, 1), (1, 1), (3, 0)):
            self.sent[k - 1, half] = value.astype(bf16)
            self.net.start(self.copies[k, half])
        else:
            self.held[{0: half, 1: 2, 3: 3}[k]] = value

    def mid(self):
        for side, key in enumerate(((1, 0), (3, 1))):
            self.copies[2, side].wait_recv()
            k, half = key
            self.sent[k - 1, half] = (self.held[2 + side] + self.far[side].astype(f32)).astype(bf16)
            self.net.start(self.copies[key])

    def finish(self):
        for key in ((1, 1), (3, 0), (1, 0), (3, 1)):
            self.copies[key].wait_recv()
        near = self.near
        return [self.held[half] + near[0, half].astype(f32) + near[1, half].astype(f32) for half in range(2)]


ORDER = (2, 1, 3, 0)


def dot(a, b, dims):
    return lax.dot_general(a, b, (dims, ((), ())), preferred_element_type=f32)


def kernel(
    start, inc, w_in, w_out, initial,
    res_out, gin_out, gout_out,
    xs, acts, us, scaled, ghs, w1, w2, slopes,
    sent, far, near, held, acc, other, zsent, zfar, zheld, znear,
    leave, arrive, totals, rowres, send, recv, local,
):
    y, x, z, c = (lax.axis_index(a) for a in ("y", "x", "z", "c"))

    barrier = pltpu.get_barrier_semaphore()
    peers = [{a: lax.rem(i + k, 4)} for a, i in (("x", x), ("y", y)) for k in (1, 2, 3)]
    peers += [{"z": lax.rem(z + k, 4)} for k in (1, 3)]
    peers += [{"c": 1 - c}] + [{"x": lax.rem(x + k, 4), "c": 1 - c} for k in (1, 2, 3)]
    for peer in peers:
        pl.semaphore_signal(barrier, inc=1, device_id=peer, device_id_type=MESH)

    locals_ = [pltpu.make_async_copy(w_in.at[:, x], w1.at[x], local.at[0])]
    for j in range(4):
        locals_.append(
            pltpu.make_async_copy(w_out.at[:, :, pl.ds(pl.multiple_of(1024 * j + x * B, B), B)], w2.at[j, x], local.at[1 + j])
        )
    for copy in locals_:
        copy.start()

    state = start[...]
    for n in range(STEPS):
        xs[pl.ds(n * B, B), place(y, B)] = state.astype(bf16)
        state = state + noise_coef * inc[n]
    norm = state * state

    net = Net(send, recv)

    def blocks(ref, n):
        return lambda owner, half: ref.at[pl.ds(n * B + half * H, H), place(owner, B)]

    def quarter(ref, first):
        if first:
            return lambda i: lambda owner, half: ref.at[i, owner, c, pl.ds(half * 64, 64)]
        return lambda i: lambda owner, half: ref.at[owner, i, c, pl.ds(half * 64, 64)]

    gx = [Gather(net, "y", blocks(xs, n)) for n in range(STEPS)]
    others = [lax.rem(x + k, 4) for k in (1, 2, 3)]
    w1s = [net.copy(w_in.at[z, i, c], w1.at[x, z, c], {"x": i}) for i in others]
    w2s = [
        net.copy(w_out.at[c, :, pl.ds(pl.multiple_of(z * 1024 + i * B, B), B)], w2.at[z, x, c], {"x": i}) for i in others
    ]
    froms = [lax.rem(x + 4 - k, 4) for k in (1, 2, 3)]
    wz1 = [Gather(net, "z", quarter(w1, True)(i)) for i in froms]
    wz2 = [Gather(net, "z", quarter(w2, False)(i)) for i in froms]
    d1 = [net.copy(w1.at[i, :, c], w1.at[i, :, c], {"c": 1 - c}) for i in froms]
    d2 = [net.copy(w2.at[:, i, c], w2.at[:, i, c], {"c": 1 - c}) for i in froms]

    def scatter(axis, k):
        return Scatter(net, axis, sent.at[k], far.at[k], near.at[k], held.at[k])

    sh = [scatter("x", n) for n in range(STEPS)]
    sz = [scatter("y", 3 + n) for n in range(STEPS)]
    sg = [scatter("x", 6 + n) for n in range(STEPS)]
    ga = [Gather(net, "x", blocks(acts, n)) for n in range(STEPS)]
    gu = [Gather(net, "y", blocks(us, n)) for n in range(STEPS)]
    gg = [Gather(net, "x", blocks(ghs, n)) for n in range(STEPS)]
    ty = [net.copy(totals.at[0, y], totals.at[0, y], {"y": lax.rem(y + k, 4)}) for k in (1, 2, 3)]
    tx = [net.copy(totals.at[1, x], totals.at[1, x], {"x": lax.rem(x + k, 4)}) for k in (1, 2, 3)]

    pl.semaphore_wait(barrier, len(peers))
    for copy in w1s:
        net.start(copy)
    gx[0].start()
    for copy in w2s:
        net.start(copy)
    gx[1].start()
    gx[2].start()

    def rows(ref, n):
        return ref[pl.ds(n * B, B), :]

    def first(n):
        for k in ORDER:
            w = w1[lax.rem(x + k, 4)].reshape(4 * B, B)
            part = dot(rows(xs, n), w, ((1,), (0,)))
            for half in range(2):
                sh[n].put(k, half, part[half * H : half * H + H])

    def second(n):
        for k in ORDER:
            w = w2[lax.rem(y + k, 4)].reshape(4 * B, B)
            part = dot(rows(acts, n), w, ((1,), (0,)))
            for half in range(2):
                sz[n].put(k, half, part[half * H : half * H + H])

    def third(n):
        for k in ORDER:
            i = lax.rem(x + k, 4)
            part = None
            for j in range(4):
                term = dot(us[pl.ds(n * B, B), pl.ds(j * B, B)], w2[j, i].reshape(B, B), ((1,), (1,)))
                part = term if part is None else part + term
            for half in range(2):
                sg[n].put(k, half, part[half * H : half * H + H])

    def activate(n):
        for half, h in enumerate(sh[n].finish()):
            sig = jax.nn.sigmoid(h)
            acts[pl.ds(n * B + half * H, H), place(x, B)] = (h * sig).astype(bf16)
            slopes[n, half] = sig * (1.0 + h * (1.0 - sig))
        ga[n].start()

    terms = [0.0, 0.0]

    def control(n):
        for half, total in enumerate(sz[n].finish()):
            zval = zscale * total
            dw = inc[n, pl.ds(half * H, H), :]
            us[pl.ds(n * B + half * H, H), place(y, B)] = (zscale * (lam_coef * time_step * zval + dw)).astype(bf16)
            term = 0.5 * lam_coef * time_step * zval * zval + zval * dw
            terms[half] = terms[half] + (term[:, :128] + term[:, 128:])
        gu[n].start()

    def hidden_grad(n):
        for half, g in enumerate(sg[n].finish()):
            r = rowres[pl.ds(half * H, H), :]
            r = jnp.concatenate([r, r], axis=1)
            ghs[pl.ds(n * B + half * H, H), place(x, B)] = (r * g * slopes[n, half]).astype(bf16)
        gg[n].start()

    for k in range(3):
        w1s[k].wait_recv()
        wz1[k].start()
    gx[0].mid()
    for k in range(3):
        wz1[k].mid()
    for k in range(3):
        w2s[k].wait_recv()
        wz2[k].start()
    gx[1].mid()
    gx[2].mid()
    for k in range(3):
        wz1[k].finish()
        net.start(d1[k])
    gx[0].finish()
    locals_[0].wait()
    for k in range(3):
        d1[k].wait_recv()
    first(0)
    for k in range(3):
        wz2[k].mid()
    gx[1].finish()
    first(1)
    sh[0].mid()
    gx[2].finish()
    first(2)
    sh[1].mid()
    activate(0)
    sh[2].mid()
    for k in range(3):
        wz2[k].finish()
        net.start(d2[k])
    activate(1)
    ga[0].mid()
    activate(2)
    ga[1].mid()
    for copy in locals_[1:]:
        copy.wait()
    for k in range(3):
        d2[k].wait_recv()
    ga[0].finish()
    second(0)
    ga[2].mid()
    ga[1].finish()
    second(1)
    sz[0].mid()
    ga[2].finish()
    second(2)
    sz[1].mid()
    control(0)
    sz[2].mid()
    control(1)
    gu[0].mid()
    control(2)

    def per_path(t):
        return jnp.sum(t.T, axis=0, keepdims=True)

    y_row = per_path(jnp.concatenate(terms, axis=0))
    n_row = per_path(norm[:, :128] + norm[:, 128:])
    totals[0, y] = jnp.concatenate([y_row, n_row, jnp.zeros((6, B), f32)], axis=0)
    for copy in ty:
        net.start(copy)
    gu[1].mid()
    gu[0].finish()
    third(0)
    for copy in ty:
        copy.wait_recv()
    totals[1, x] = totals[0, 0] + totals[0, 1] + totals[0, 2] + totals[0, 3]
    for copy in tx:
        net.start(copy)
    gu[2].mid()
    gu[1].finish()
    third(1)
    sg[0].mid()
    for copy in tx:
        copy.wait_recv()
    both = totals[1, 0] + totals[1, 1] + totals[1, 2] + totals[1, 3]
    residual = initial[0] + both[0:1] - jnp.log((1.0 + both[1:2]) * 0.5)
    res_out[...] = residual
    rowres[...] = jnp.broadcast_to(residual, (128, B)).T
    gu[2].finish()
    third(2)
    sg[1].mid()
    hidden_grad(0)
    sg[2].mid()
    hidden_grad(1)
    gg[0].mid()

    swap = {}
    zs = []
    for g in range(2):
        for k in ORDER:
            cols = place(lax.rem(z + k, 4), B)
            for e in range(2):
                swap[g, k, e] = net.copy(acc.at[g, 2 * (1 - c) + e, :, cols], other.at[g, e, :, cols], {"c": 1 - c})
        zs.append(Scatter(net, "z", zsent.at[g], zfar.at[g], znear.at[g], zheld.at[g]))

    def exchange(g):
        for k in ORDER:
            for e in range(2):
                net.start(swap[g, k, e])

    def over_z(g):
        for k in ORDER:
            cols = place(lax.rem(z + k, 4), B)
            for e in range(2):
                swap[g, k, e].wait_recv()
                zs[g].put(k, e, acc[g, 2 * c + e, :, cols] + other[g, e, :, cols])

    def to_owner(g):
        outs = []
        for e, value in enumerate(zs[g].finish()):
            value = value.T if g == 0 else value
            i = 2 * c + e
            leave[g, e] = value
            outs.append(
                pltpu.make_async_remote_copy(
                    src_ref=leave.at[g, e],
                    dst_ref=arrive.at[g, lax.rem(x, 2)],
                    send_sem=send.at[COPIES + 2 * g + e],
                    recv_sem=recv.at[COPIES + 2 * g + lax.rem(x, 2)],
                    device_id={"x": i, "c": x // 2},
                    device_id_type=MESH,
                )
            )

            @pl.when(i != x)
            def _(copy=outs[e]):
                copy.start()

            @pl.when(i == x)
            def _(e=e):
                arrive[g, e] = leave[g, e]

        return outs

    def collect(g, outs):
        target = (gin_out, gout_out)[g]
        puts = []
        for t in range(2):

            @pl.when(2 * c + t != x)
            def _(t=t):
                pltpu.make_async_remote_copy(
                    src_ref=leave.at[g, t],
                    dst_ref=arrive.at[g, t],
                    send_sem=send.at[COPIES + 2 * g + t],
                    recv_sem=recv.at[COPIES + 2 * g + t],
                    device_id={"x": 2 * c + t, "c": x // 2},
                    device_id_type=MESH,
                ).wait_recv()

            dst = target.at[pl.ds(t * B, B), :] if g == 0 else target.at[:, pl.ds(t * B, B)]
            copy = pltpu.make_async_copy(arrive.at[g, t], dst, local.at[8 + 2 * g + t])
            copy.start()
            puts.append(copy)
        for e in range(2):

            @pl.when(2 * c + e != x)
            def _(copy=outs[e]):
                copy.wait_send()

        return puts

    halves = [2 * (1 - c), 2 * (1 - c) + 1, 2 * c, 2 * c + 1]
    for n in range(STEPS):
        for k in range(8):
            lanes = pl.ds(k * 128, 128)
            scaled[pl.ds(n * B, B), lanes] = (us[pl.ds(n * B, B), lanes].astype(f32) * rowres[...]).astype(bf16)
    for i in halves:
        acc[1, i] = dot(acts[:, place(i, B)], scaled[...], ((0,), (0,)))
    exchange(1)
    hidden_grad(2)
    gg[1].mid()
    over_z(1)
    gg[0].finish()
    gg[1].finish()
    gg[2].mid()
    two = pl.ds(0, 2 * B)
    for i in halves:
        acc[0, i] = dot(ghs[two, place(i, B)], xs[two, :], ((0,), (0,)))
    zs[1].mid()
    gg[2].finish()
    last = pl.ds(2 * B, B)
    for i in halves:
        acc[0, i] += dot(ghs[last, place(i, B)], xs[last, :], ((0,), (0,)))
    exchange(0)
    over_z(0)
    outs1 = to_owner(1)
    zs[0].mid()
    puts = collect(1, outs1)
    outs0 = to_owner(0)
    puts += collect(0, outs0)
    for copy in puts:
        copy.wait()
    net.drain()


def on_device(start, increments, w_in, w_out, initial):
    vmem, anywhere = pl.BlockSpec(memory_space=pltpu.VMEM), pl.BlockSpec(memory_space=pl.ANY)
    stacked = pltpu.VMEM((STEPS * B, 4 * B), bf16)
    weights = pltpu.VMEM((4, 4, 2, H, B), bf16)
    residual, grad_in, grad_out = pl.pallas_call(
        kernel,
        out_shape=(
            jax.ShapeDtypeStruct((1, B), f32),
            jax.ShapeDtypeStruct((2 * B, B), f32),
            jax.ShapeDtypeStruct((B, 2 * B), f32),
        ),
        in_specs=[vmem, vmem, anywhere, anywhere, pl.BlockSpec(memory_space=pltpu.SMEM)],
        out_specs=(vmem, anywhere, anywhere),
        scratch_shapes=[
            stacked,
            stacked,
            stacked,
            stacked,
            stacked,
            weights,
            weights,
            pltpu.VMEM((STEPS, 2, H, B), f32),
            pltpu.VMEM((9, 3, 2, H, B), bf16),
            pltpu.VMEM((9, 2, H, B), bf16),
            pltpu.VMEM((9, 2, 2, H, B), bf16),
            pltpu.VMEM((9, 4, H, B), f32),
            pltpu.VMEM((2, 4, B, 4 * B), f32),
            pltpu.VMEM((2, 2, B, 4 * B), f32),
            pltpu.VMEM((2, 3, 2, B, B), bf16),
            pltpu.VMEM((2, 2, B, B), bf16),
            pltpu.VMEM((2, 4, B, B), f32),
            pltpu.VMEM((2, 2, 2, B, B), bf16),
            pltpu.VMEM((2, 2, B, B), f32),
            pltpu.VMEM((2, 2, B, B), f32),
            pltpu.VMEM((2, 4, 8, B), f32),
            pltpu.VMEM((B, 128), f32),
            pltpu.SemaphoreType.DMA((COPIES + 4,)),
            pltpu.SemaphoreType.DMA((COPIES + 4,)),
            pltpu.SemaphoreType.DMA((12,)),
        ],
        compiler_params=pltpu.CompilerParams(collective_id=0, has_side_effects=True, vmem_limit_bytes=66000000),
    )(start, increments, w_in.reshape(4, 4, 2, H, B), w_out.reshape(2, H, D), initial.reshape(1))
    return residual.reshape(B), grad_in, grad_out


def solution(mesh):
    finer = Mesh(mesh.devices.reshape(4, 4, 4, 2), ("y", "x", "z", "c"))
    return jax.shard_map(
        on_device,
        mesh=finer,
        in_specs=(P(BATCH, DIM), P(None, BATCH, DIM), P(None, DIM), P(DIM, None), P()),
        out_specs=(P(BATCH), P(BATCH, DIM), P(DIM, BATCH)),
        check_vma=False,
    )
```

```python
import math

import jax
import jax.numpy as jnp
from jax import lax
from jax.experimental import pallas as pl
from jax.experimental.pallas import tpu as pltpu
from jax.sharding import Mesh
from jax.sharding import PartitionSpec as P

D = 4096
STEPS = 3
B = 256
H = B // 2
DIM = ("y", "x")
BATCH = ("z", "c")
MESH = pl.DeviceIdType.MESH
f32, bf16 = jnp.float32, jnp.bfloat16

time_step = 1.0 / 64.0
lam_coef = 50.0
noise_coef = math.sqrt(2.0)
zscale = 2.0 / math.sqrt(D)
COPIES = 250


def place(pos, extent):
    return pl.ds(pl.multiple_of(pos * extent, extent), extent)


class Net:
    def __init__(self, send, recv):
        self.send, self.recv, self.count, self.begun, self.seen = send, recv, 0, [], set()

    def copy(self, src, dst, device):
        k = self.count
        self.count += 1
        assert self.count <= COPIES
        return pltpu.make_async_remote_copy(
            src_ref=src,
            dst_ref=dst,
            send_sem=self.send.at[k],
            recv_sem=self.recv.at[k],
            device_id=device,
            device_id_type=MESH,
        )

    def start(self, copy):
        copy.start()
        self.begun.append(copy)

    def arrived(self, copy):
        if id(copy) not in self.seen:
            self.seen.add(id(copy))
            copy.wait_recv()

    def drain(self):
        for copy in self.begun:
            copy.wait_send()


class Gather:
    def __init__(self, net, axis, view):
        p = lax.axis_index(axis)
        r, l = lax.rem(p + 1, 4), lax.rem(p + 3, 4)
        self.net = net
        self.copies = [
            net.copy(view(owner, half), view(owner, half), {axis: to})
            for owner, half, to in ((p, 0, r), (p, 1, l), (p, 1, r), (p, 0, l), (l, 0, r), (r, 1, l))
        ]

    def start(self):
        for k in range(4):
            self.net.start(self.copies[k])

    def mid(self):
        for k in range(2):
            self.net.arrived(self.copies[k])
            self.net.start(self.copies[4 + k])

    def finish(self):
        for k in range(2, 6):
            self.net.arrived(self.copies[k])


class Scatter:
    def __init__(self, net, axis, sent, far, near, held):
        p = lax.axis_index(axis)
        r, l = {axis: lax.rem(p + 1, 4)}, {axis: lax.rem(p + 3, 4)}
        self.net, self.sent, self.far, self.near, self.held = net, sent, far, near, held
        self.copies = {
            (2, 0): net.copy(sent.at[1, 0], far.at[0], r),
            (2, 1): net.copy(sent.at[1, 1], far.at[1], l),
            (1, 1): net.copy(sent.at[0, 1], near.at[0, 1], r),
            (3, 0): net.copy(sent.at[2, 0], near.at[1, 0], l),
            (1, 0): net.copy(sent.at[0, 0], near.at[0, 0], r),
            (3, 1): net.copy(sent.at[2, 1], near.at[1, 1], l),
        }

    def put(self, k, half, value):
        if (k, half) in ((2, 0), (2, 1), (1, 1), (3, 0)):
            self.sent[k - 1, half] = value.astype(bf16)
            self.net.start(self.copies[k, half])
        else:
            self.held[{0: half, 1: 2, 3: 3}[k]] = value

    def mid(self):
        for side, key in enumerate(((1, 0), (3, 1))):
            self.copies[2, side].wait_recv()
            k, half = key
            self.sent[k - 1, half] = (self.held[2 + side] + self.far[side].astype(f32)).astype(bf16)
            self.net.start(self.copies[key])

    def finish(self):
        for key in ((1, 1), (3, 0), (1, 0), (3, 1)):
            self.copies[key].wait_recv()
        near = self.near
        return [self.held[half] + near[0, half].astype(f32) + near[1, half].astype(f32) for half in range(2)]


ORDER = (2, 1, 3, 0)
PROGRAM = [
    "w1a2", "gx0.mid", "w1a1", "w1a0", "w1b1", "w1b2", "w1b0", "w2a1", "gx1.mid", "gx2.mid", "w1c1", "w1c2", "f02",
    "w2b1", "w2a2", "w1c0", "f01", "f12", "f03", "sh0.mid", "w2a0", "f11", "f13", "w2b0", "w2b2", "w2c1", "sh1.mid",
    "f00", "f10", "act0", "ga0.mid", "w2c2", "act1", "w2c0", "s02", "s03", "s01", "ga1.mid", "f22", "f21", "s00",
    "sz0.mid", "f20", "f23", "s12", "s13", "sh2.mid", "s11", "sz1.mid", "con0", "s10", "act2", "con1", "ga2.mid",
    "gu0.mid", "s22", "s23", "s21", "t02", "sz2.mid", "t01", "s20", "t00", "gu1.mid", "t03", "con2", "sg0.mid", "t12",
    "t13", "t11", "tot", "gu2.mid", "sg1.mid", "tot2", "t22", "t23", "t21", "res", "hid0", "sc0", "t10", "sc1", "t20",
    "sg2.mid", "sc2", "hid1", "go1", "gg0.mid", "go2", "po0", "po2", "po3", "hid2", "gg1.mid", "po1", "gg2.mid",
    "zo.mid", "gi1", "gi2", "gi3", "pi2", "pi1", "pi3", "zi.mid", "zo.fin", "pi0", "zi.fin", "colo", "coli",
]


def dot(a, b, dims):
    return lax.dot_general(a, b, (dims, ((), ())), preferred_element_type=f32)


def kernel(
    start_in, inc_in, w_in, w_out, initial,
    res_out, grads_out,
    start, inc, xs, acts, us, scaled, ghs, w1, w2, slopes,
    sent, far, near, held, acc, other, zsent, zfar, zheld, znear,
    leave, totals, nrow, folded, rowres, send, recv, local,
):
    y, x, z, c = (lax.axis_index(a) for a in ("y", "x", "z", "c"))

    barrier = pltpu.get_barrier_semaphore()
    peers = [{a: lax.rem(i + k, 4)} for a, i in (("x", x), ("y", y)) for k in (1, 2, 3)]
    peers += [{"z": lax.rem(z + k, 4)} for k in (1, 3)]
    peers += [{"c": 1 - c}] + [{"x": lax.rem(x + k, 4), "c": 1 - c} for k in (1, 2, 3)]
    for peer in peers:
        pl.semaphore_signal(barrier, inc=1, device_id=peer, device_id_type=MESH)

    fetch = [pltpu.make_async_copy(start_in, start, local.at[0])]
    fetch += [pltpu.make_async_copy(inc_in.at[n], inc.at[n], local.at[1 + n]) for n in range(STEPS)]
    own1 = [pltpu.make_async_copy(w_in.at[:, x], w1.at[x], local.at[4])]
    own2 = []
    for j in range(4):
        cols = pl.ds(pl.multiple_of(1024 * j + x * B, B), B)
        own2.append(pltpu.make_async_copy(w_out.at[:, :, cols], w2.at[j, x], local.at[5 + j]))
    for copy in fetch + own1 + own2:
        copy.start()

    net = Net(send, recv)

    def blocks(ref, n):
        return lambda owner, half: ref.at[pl.ds(n * B + half * H, H), place(owner, B)]

    def piece(m, i, j):
        return w1.at[i, j, c] if m == 1 else w2.at[j, i, c]

    def quarter(m, i):
        return lambda owner, half: piece(m, i, owner).at[pl.ds(half * 64, 64)]

    gx = [Gather(net, "y", blocks(xs, n)) for n in range(STEPS)]
    others = [lax.rem(x + k, 4) for k in (1, 2, 3)]
    froms = [lax.rem(x + 4 - k, 4) for k in (1, 2, 3)]
    ws, wz, wd = {}, {}, {}
    for m in (1, 2):
        for k, i in enumerate(others):
            cols = pl.ds(pl.multiple_of(z * 1024 + i * B, B), B)
            src = w_in.at[z, i, c] if m == 1 else w_out.at[c, :, cols]
            ws[m, k] = net.copy(src, piece(m, x, z), {"x": i})
        for k, i in enumerate(froms):
            wz[m, k] = Gather(net, "z", quarter(m, i))
            for t in range(4):
                mine = piece(m, i, lax.rem(z + t, 4))
                wd[m, k, t] = net.copy(mine, mine, {"c": 1 - c})

    def scatter(axis, k):
        return Scatter(net, axis, sent.at[k], far.at[k], near.at[k], held.at[k])

    sh = [scatter("x", n) for n in range(STEPS)]
    sz = [scatter("y", 3 + n) for n in range(STEPS)]
    sg = [scatter("x", 6 + n) for n in range(STEPS)]
    ga = [Gather(net, "x", blocks(acts, n)) for n in range(STEPS)]
    gu = [Gather(net, "y", blocks(us, n)) for n in range(STEPS)]
    gg = [Gather(net, "x", blocks(ghs, n)) for n in range(STEPS)]
    ty = [net.copy(totals.at[0, y], totals.at[0, y], {"y": lax.rem(y + k, 4)}) for k in (1, 2, 3)]
    tx = [net.copy(totals.at[1, x], totals.at[1, x], {"x": lax.rem(x + k, 4)}) for k in (1, 2, 3)]
    swap, zs = {}, []
    for g in range(2):
        for k in ORDER:
            cols = place(lax.rem(z + k, 4), B)
            for e in range(2):
                swap[g, k, e] = net.copy(acc.at[g, 2 * (1 - c) + e, :, cols], other.at[g, e, :, cols], {"c": 1 - c})
        zs.append(Scatter(net, "z", zsent.at[g], zfar.at[g], znear.at[g], zheld.at[g]))

    def per_path(t):
        return jnp.sum(t.T, axis=0, keepdims=True)

    pl.semaphore_wait(barrier, len(peers))
    for k in (1, 0, 2):
        net.start(ws[1, k])
    fetch[0].wait()
    state = start[...]
    for n in range(STEPS):
        xs[pl.ds(n * B, B), place(y, B)] = state.astype(bf16)
        gx[n].start()
        if n == 0:
            for k in (1, 0, 2):
                net.start(ws[2, k])
        fetch[1 + n].wait()
        state = state + noise_coef * inc[n]
    norm = state * state
    nrow[...] = per_path(norm[:, :128] + norm[:, 128:])

    def rows(ref, n):
        return ref[pl.ds(n * B, B), :]

    def put_both(scatter_sum, k, part):
        for half in range(2):
            scatter_sum.put(k, half, part[half * H : half * H + H])

    ready = set()

    def wait_once(copies):
        for copy in copies:
            if id(copy) not in ready:
                ready.add(id(copy))
                copy.wait()

    def weights(m, k):
        net.arrived(ws[m, k])
        for copy in wz[m, k].copies:
            net.arrived(copy)
        for t in range(4):
            net.arrived(wd[m, k, t])

    def first(n, k):
        gx[n].finish()
        if k:
            weights(1, 3 - k)
        else:
            wait_once(own1)
        w = w1[lax.rem(x + k, 4)].reshape(4 * B, B)
        put_both(sh[n], k, dot(rows(xs, n), w, ((1,), (0,))))

    def second(n, k):
        ga[n].finish()
        for e in range(3):
            weights(2, e)
        wait_once(own2)
        w = w2[lax.rem(y + k, 4)].reshape(4 * B, B)
        put_both(sz[n], k, dot(rows(acts, n), w, ((1,), (0,))))

    def third(n, k):
        gu[n].finish()
        i = lax.rem(x + k, 4)
        part = None
        for j in range(4):
            term = dot(us[pl.ds(n * B, B), pl.ds(j * B, B)], w2[j, i].reshape(B, B), ((1,), (1,)))
            part = term if part is None else part + term
        put_both(sg[n], k, part)

    def activate(n):
        for half, h in enumerate(sh[n].finish()):
            sig = jax.nn.sigmoid(h)
            acts[pl.ds(n * B + half * H, H), place(x, B)] = (h * sig).astype(bf16)
            slopes[n, half] = sig * (1.0 + h * (1.0 - sig))
        ga[n].start()

    begun = []

    def control(n):
        for half, total in enumerate(sz[n].finish()):
            zval = zscale * total
            dw = inc[n, pl.ds(half * H, H), :]
            us[pl.ds(n * B + half * H, H), place(y, B)] = (zscale * (lam_coef * time_step * zval + dw)).astype(bf16)
            term = 0.5 * lam_coef * time_step * zval * zval + zval * dw
            term = term[:, :128] + term[:, 128:]
            folded[half] = folded[half] + term if begun else term
        begun.append(n)
        gu[n].start()

    def hidden_grad(n):
        for half, g in enumerate(sg[n].finish()):
            r = rowres[pl.ds(half * H, H), :]
            r = jnp.concatenate([r, r], axis=1)
            ghs[pl.ds(n * B + half * H, H), place(x, B)] = (r * g * slopes[n, half]).astype(bf16)
        gg[n].start()

    def totals_y():
        y_row = per_path(folded[...].reshape(B, 128))
        totals[0, y] = jnp.concatenate([y_row, nrow[...], jnp.zeros((6, B), f32)], axis=0)
        for copy in ty:
            net.start(copy)

    def totals_x():
        for copy in ty:
            net.arrived(copy)
        totals[1, x] = totals[0, 0] + totals[0, 1] + totals[0, 2] + totals[0, 3]
        for copy in tx:
            net.start(copy)

    def residuals():
        for copy in tx:
            net.arrived(copy)
        both = totals[1, 0] + totals[1, 1] + totals[1, 2] + totals[1, 3]
        residual = initial[0] + both[0:1] - jnp.log((1.0 + both[1:2]) * 0.5)
        res_out[...] = residual
        rowres[...] = jnp.broadcast_to(residual, (128, B)).T

    def scale(n):
        gu[n].finish()
        for k in range(8):
            lanes = pl.ds(k * 128, 128)
            scaled[pl.ds(n * B, B), lanes] = (us[pl.ds(n * B, B), lanes].astype(f32) * rowres[...]).astype(bf16)

    def give(g):
        for k in ORDER:
            for e in range(2):
                net.start(swap[g, k, e])

    def out_sum(core):
        for e in range(2):
            i = 2 * core + e
            acc[1, i] = dot(acts[:, place(i, B)], scaled[...], ((0,), (0,)))

    def in_sum(core, first_row, extent):
        span = pl.ds(first_row, extent)
        for e in range(2):
            i = 2 * core + e
            part = dot(ghs[span, place(i, B)], xs[span, :], ((0,), (0,)))
            acc[0, i] = acc[0, i] + part if first_row else part

    def over_z(g, k):
        cols = place(lax.rem(z + k, 4), B)
        for e in range(2):
            net.arrived(swap[g, k, e])
            zs[g].put(k, e, acc[g, 2 * c + e, :, cols] + other[g, e, :, cols])

    def leaving(g, e, slot):
        return pltpu.make_async_remote_copy(
            src_ref=leave.at[g, e],
            dst_ref=grads_out.at[g, slot],
            send_sem=send.at[COPIES + 2 * g + e],
            recv_sem=recv.at[COPIES + 2 * g + slot],
            device_id={"x": 2 * c + e, "c": x // 2},
            device_id_type=MESH,
        )

    def staying(g, e):
        return pltpu.make_async_copy(leave.at[g, e], grads_out.at[g, e], local.at[9 + 2 * g + e])

    def to_owner(g):
        for e, value in enumerate(zs[g].finish()):
            leave[g, e] = (value.T if g == 0 else value).astype(bf16)

            @pl.when(2 * c + e != x)
            def _(e=e):
                leaving(g, e, lax.rem(x, 2)).start()

            @pl.when(2 * c + e == x)
            def _(e=e):
                staying(g, e).start()

    def collect(g):
        for e in range(2):

            @pl.when(2 * c + e != x)
            def _(e=e):
                copy = leaving(g, e, e)
                copy.wait_recv()
                copy.wait_send()

            @pl.when(2 * c + e == x)
            def _(e=e):
                staying(g, e).wait()

    def weights_in(m, k):
        net.arrived(ws[m, k])
        wz[m, k].start()
        net.start(wd[m, k, 0])

    def weights_out(m, k):
        wz[m, k].finish()
        for t in (1, 3, 2):
            net.start(wd[m, k, t])

    tasks = {"tot": totals_y, "tot2": totals_x, "res": residuals}
    for m in (1, 2):
        for k in range(3):
            tasks[f"w{m}a{k}"] = lambda m=m, k=k: weights_in(m, k)
            tasks[f"w{m}b{k}"] = wz[m, k].mid
            tasks[f"w{m}c{k}"] = lambda m=m, k=k: weights_out(m, k)
    for n in range(STEPS):
        for k in range(4):
            tasks[f"f{n}{k}"] = lambda n=n, k=k: first(n, k)
            tasks[f"s{n}{k}"] = lambda n=n, k=k: second(n, k)
            tasks[f"t{n}{k}"] = lambda n=n, k=k: third(n, k)
        named = {"gx": gx, "sh": sh, "ga": ga, "sz": sz, "gu": gu, "sg": sg, "gg": gg}
        for name, ops in named.items():
            tasks[f"{name}{n}.mid"] = ops[n].mid
        tasks[f"act{n}"] = lambda n=n: activate(n)
        tasks[f"con{n}"] = lambda n=n: control(n)
        tasks[f"hid{n}"] = lambda n=n: hidden_grad(n)
        tasks[f"sc{n}"] = lambda n=n: scale(n)

    def go1():
        out_sum(1 - c)
        give(1)

    def gi1():
        for n in range(2):
            gg[n].finish()
        for core in (1 - c, c):
            in_sum(core, 0, 2 * B)

    def gi2():
        gg[2].finish()
        in_sum(1 - c, 2 * B, B)
        give(0)

    tasks |= {"go1": go1, "go2": lambda: out_sum(c), "gi1": gi1, "gi2": gi2, "gi3": lambda: in_sum(c, 2 * B, B)}
    for g, name in enumerate("io"):
        for k in range(4):
            tasks[f"p{name}{k}"] = lambda g=g, k=k: over_z(g, k)
        tasks[f"z{name}.mid"] = zs[g].mid
        tasks[f"z{name}.fin"] = lambda g=g: to_owner(g)
        tasks[f"col{name}"] = lambda g=g: collect(g)

    assert sorted(PROGRAM) == sorted(tasks)
    for name in PROGRAM:
        with jax.named_scope(name):
            tasks[name]()
    net.drain()


def placing(row, blocks, residual, grad_in, grad_out):
    residual[...] = row[...].reshape(B)
    for t in range(2):
        grad_in[pl.ds(t * B, B), :] = blocks[0, t].astype(f32)
        grad_out[:, pl.ds(t * B, B)] = blocks[1, t].astype(f32)


def on_device(start, increments, w_in, w_out, initial):
    vmem, anywhere = pl.BlockSpec(memory_space=pltpu.VMEM), pl.BlockSpec(memory_space=pl.ANY)
    stacked = pltpu.VMEM((STEPS * B, 4 * B), bf16)
    weights = pltpu.VMEM((4, 4, 2, H, B), bf16)
    row, blocks = pl.pallas_call(
        kernel,
        out_shape=(jax.ShapeDtypeStruct((1, B), f32), jax.ShapeDtypeStruct((2, 2, B, B), bf16)),
        in_specs=[anywhere] * 4 + [pl.BlockSpec(memory_space=pltpu.SMEM)],
        out_specs=(vmem, anywhere),
        scratch_shapes=[
            pltpu.VMEM((B, B), f32),
            pltpu.VMEM((STEPS, B, B), f32),
            stacked,
            stacked,
            stacked,
            stacked,
            stacked,
            weights,
            weights,
            pltpu.VMEM((STEPS, 2, H, B), f32),
            pltpu.VMEM((9, 3, 2, H, B), bf16),
            pltpu.VMEM((9, 2, H, B), bf16),
            pltpu.VMEM((9, 2, 2, H, B), bf16),
            pltpu.VMEM((9, 4, H, B), f32),
            pltpu.VMEM((2, 4, B, 4 * B), f32),
            pltpu.VMEM((2, 2, B, 4 * B), f32),
            pltpu.VMEM((2, 3, 2, B, B), bf16),
            pltpu.VMEM((2, 2, B, B), bf16),
            pltpu.VMEM((2, 4, B, B), f32),
            pltpu.VMEM((2, 2, 2, B, B), bf16),
            pltpu.VMEM((2, 2, B, B), bf16),
            pltpu.VMEM((2, 4, 8, B), f32),
            pltpu.VMEM((1, B), f32),
            pltpu.VMEM((2, H, 128), f32),
            pltpu.VMEM((B, 128), f32),
            pltpu.SemaphoreType.DMA((COPIES + 4,)),
            pltpu.SemaphoreType.DMA((COPIES + 4,)),
            pltpu.SemaphoreType.DMA((13,)),
        ],
        compiler_params=pltpu.CompilerParams(collective_id=0, has_side_effects=True, vmem_limit_bytes=66000000),
    )(start, increments, w_in.reshape(4, 4, 2, H, B), w_out.reshape(2, H, D), initial.reshape(1))
    return pl.pallas_call(
        placing,
        out_shape=(
            jax.ShapeDtypeStruct((B,), f32),
            jax.ShapeDtypeStruct((2 * B, B), f32),
            jax.ShapeDtypeStruct((B, 2 * B), f32),
        ),
        in_specs=[vmem, vmem],
        out_specs=(vmem, vmem, vmem),
    )(row, blocks)


def solution(mesh):
    finer = Mesh(mesh.devices.reshape(4, 4, 4, 2), ("y", "x", "z", "c"))
    return jax.shard_map(
        on_device,
        mesh=finer,
        in_specs=(P(BATCH, DIM), P(None, BATCH, DIM), P(None, DIM), P(DIM, None), P()),
        out_specs=(P(BATCH), P(BATCH, DIM), P(DIM, BATCH)),
        check_vma=False,
    )
```

```python
import math

import jax
import jax.numpy as jnp
from jax import lax
from jax.experimental import pallas as pl
from jax.experimental.pallas import tpu as pltpu
from jax.sharding import Mesh
from jax.sharding import PartitionSpec as P

D = 4096
STEPS = 3
B = 256
H = B // 2
Q = B // 4
CHAINS = 2 * STEPS
DIM = ("y", "x")
BATCH = ("z", "c")
MESH = pl.DeviceIdType.MESH
f32, bf16 = jnp.float32, jnp.bfloat16

time_step = 1.0 / 64.0
lam_coef = 50.0
noise_coef = math.sqrt(2.0)
zscale = 2.0 / math.sqrt(D)
ARRIVALS = 170
LEAVING = 48


def place(pos, extent):
    return pl.ds(pl.multiple_of(pos * extent, extent), extent)


class Net:

    def __init__(self, send, recv):
        self.send, self.recv, self.count, self.begun, self.seen = send, recv, 0, [], set()

    def slots(self, count):
        self.count += count
        assert self.count <= ARRIVALS
        return [self.recv.at[k] for k in range(self.count - count, self.count)]

    def copy(self, src, dst, device, slot=None):
        return (src, dst, device, self.slots(1)[0] if slot is None else slot)

    def made(self, copy, send):
        src, dst, device, slot = copy
        return pltpu.make_async_remote_copy(
            src_ref=src, dst_ref=dst, send_sem=send, recv_sem=slot, device_id=device, device_id_type=MESH
        )

    def start(self, copy):
        send = self.send.at[len(self.begun) % LEAVING]
        if len(self.begun) >= LEAVING:
            self.begun[len(self.begun) - LEAVING].wait_send()
        made = self.made(copy, send)
        made.start()
        self.begun.append(made)

    def arrived(self, copy):
        if id(copy) not in self.seen:
            self.seen.add(id(copy))
            self.made(copy, self.send.at[0]).wait_recv()

    def drain(self):
        for copy in self.begun[-LEAVING:]:
            copy.wait_send()


class Gather:

    def __init__(self, net, axis, view, four, slots=None):
        p = lax.axis_index(axis)
        r, l = lax.rem(p + 1, 4), lax.rem(p + 3, 4)
        self.net, self.slots = net, slots or net.slots(3)
        self.copies = [
            net.copy(view(owner, half), view(owner, half), {axis: to}, self.slots[min(k, 2)])
            for k, (owner, half, to) in enumerate(((p, 0, r), (p, 1, l), (p, 1, r), (p, 0, l), (l, 0, r), (r, 1, l)))
        ]
        self.rest = (four, four, {axis: r}, self.slots[2])

    def start(self):
        for k in range(4):
            self.net.start(self.copies[k])

    def mid(self):
        for k in range(2):
            self.net.arrived(self.copies[k])
            self.net.start(self.copies[4 + k])

    def finish(self):
        self.net.arrived(self.rest)


class Scatter:

    def __init__(self, net, axis, sent, far, near, held, slots=None):
        p = lax.axis_index(axis)
        r, l = {axis: lax.rem(p + 1, 4)}, {axis: lax.rem(p + 3, 4)}
        self.net, self.sent, self.far, self.near, self.held = net, sent, far, near, held
        self.slots = slots or net.slots(3)
        a, b, rest = self.slots
        self.copies = {
            (2, 0): net.copy(sent.at[1, 0], far.at[0], r, a),
            (2, 1): net.copy(sent.at[1, 1], far.at[1], l, b),
            (1, 1): net.copy(sent.at[0, 1], near.at[0, 1], r, rest),
            (3, 0): net.copy(sent.at[2, 0], near.at[1, 0], l, rest),
            (1, 0): net.copy(sent.at[0, 0], near.at[0, 0], r, rest),
            (3, 1): net.copy(sent.at[2, 1], near.at[1, 1], l, rest),
        }
        self.rest = (near, near, r, rest)

    def put(self, k, half, value):
        if (k, half) in ((2, 0), (2, 1), (1, 1), (3, 0)):
            self.sent[k - 1, half] = value.astype(bf16)
            self.net.start(self.copies[k, half])
        else:
            self.held[{0: half, 1: 2, 3: 3}[k]] = value

    def mid(self):
        for side, key in enumerate(((1, 0), (3, 1))):
            self.net.arrived(self.copies[2, side])
            k, half = key
            self.sent[k - 1, half] = (self.held[2 + side] + self.far[side].astype(f32)).astype(bf16)
            self.net.start(self.copies[key])

    def finish(self):
        self.net.arrived(self.rest)
        near = self.near
        return [self.held[half] + near[0, half].astype(f32) + near[1, half].astype(f32) for half in range(2)]


ORDER = (2, 1, 3, 0)
PROGRAM = [
    "w1a2", "gx0.mid", "w1a1", "w1a0", "w1b1", "w1b2", "gx2.mid", "gx3.mid", "w1b0", "w2a2", "w1c1", "gx1.mid",
    "gx5.mid", "w2a1", "gx4.mid", "w1c2", "f22", "w1c0", "f32", "f20", "w2b2", "f02", "f21", "f12", "f10", "w2a0",
    "f23", "f40", "sh2.mid", "f31", "f33", "w2b1", "sh3.mid", "f01", "f03", "f50", "f00", "w2b0", "sh0.mid", "w2c2",
    "f30", "act2", "w2c1", "act3", "ga2.mid", "act0", "w2c0", "ga3.mid", "f11", "f13", "sh1.mid", "s22", "s21", "s23",
    "ga0.mid", "f42", "f52", "f43", "f41", "s32", "s31", "sz2.mid", "act1", "s33", "s20", "s02", "s01", "sh4.mid",
    "f51", "sz3.mid", "f53", "s03", "sh5.mid", "con2", "s30", "ga1.mid", "s00", "sz0.mid", "act4", "con3", "act5",
    "gu2.mid", "s12", "con0", "ga4.mid", "s11", "gu3.mid", "s13", "ga5.mid", "sz1.mid", "t22", "s42", "s41",
    "gu0.mid", "s43", "s10", "s52", "s40", "con1", "t32", "sz4.mid", "t31", "s53", "t21", "s51", "s50", "t33",
    "sz5.mid", "t02", "t23", "gu1.mid", "sg2.mid", "t00", "t20", "con4", "t03", "t01", "con5", "t30", "t12",
    "sg3.mid", "tot", "sg0.mid", "t13", "gu4.mid", "t11", "gu5.mid", "sg1.mid", "tot2", "t42", "t43", "t41", "t53",
    "t51", "t40", "t52", "sg4.mid", "res", "hid0", "hid2", "resp", "sc5", "sc4", "sc3", "sc2", "hid3", "sc0", "sc1",
    "go1", "hid4", "go0", "t10", "po11", "hid1", "t50", "gg3.mid", "po01", "po02", "sg5.mid", "gg0.mid", "gg2.mid",
    "po13", "gg4.mid", "po03", "gs3", "gg1.mid", "po12", "hid5", "gs0", "po00", "gs2", "gs4", "gs1", "gg5.mid", "gi0",
    "zo0.mid", "zo1.mid", "gs5", "gi1", "gj0", "gj1", "pi02", "po10", "pi12", "pi01", "pi00", "pi03", "zo1.fin",
    "zo0.fin", "zi0.mid", "pi11", "pi13", "pi10", "zi1.mid", "zi0.fin", "zi1.fin", "colo", "coli",
]


def dot(a, b, dims):
    return lax.dot_general(a, b, (dims, ((), ())), preferred_element_type=f32)


def kernel(
    start_in, inc_in, w_in, w_out, initial_in,
    res_out, grads_out,
    start, inc, xs, us, acts, scaled, ghs, w1, w2, slopes,
    sent, far, near, held, acc, zsent, zfar, zheld, znear,
    leave, totals, nrow, folded, resrow, rowres, give1, give2, initial, send, recv, local,
):
    y, x, z, c = (lax.axis_index(a) for a in ("y", "x", "z", "c"))

    barrier = pltpu.get_barrier_semaphore()
    peers = [{a: lax.rem(i + k, 4)} for a, i in (("x", x), ("y", y)) for k in (1, 2, 3)]
    peers += [{"z": lax.rem(z + k, 4)} for k in (1, 3)]
    peers += [{"c": 1 - c}] + [{"x": lax.rem(x + k, 4), "c": 1 - c} for k in (1, 2, 3)]
    for peer in peers:
        pl.semaphore_signal(barrier, inc=1, device_id=peer, device_id_type=MESH)

    fetch = [pltpu.make_async_copy(start_in, start, local.at[0])]
    fetch += [pltpu.make_async_copy(inc_in.at[n], inc.at[n], local.at[1 + n]) for n in range(STEPS)]
    own1 = [pltpu.make_async_copy(w_in.at[:, x], w1.at[x], local.at[4])]
    own2 = []
    for j in range(4):
        cols = pl.ds(pl.multiple_of(1024 * j + x * B, B), B)
        own2.append(pltpu.make_async_copy(w_out.at[:, :, cols], w2.at[j, x], local.at[5 + j]))
    gift1 = pltpu.make_async_copy(w_in.at[z, :, c], give1, local.at[9])
    gift2 = pltpu.make_async_copy(w_out.at[c, :, pl.ds(pl.multiple_of(z * 1024, 1024), 1024)], give2, local.at[10])
    scalar = pltpu.make_async_copy(initial_in, initial, local.at[11])
    for copy in [gift1] + fetch + [gift2] + own1 + own2 + [scalar]:
        copy.start()

    net = Net(send, recv)
    partner = {"c": 1 - c}

    def states_of(ref, n):
        return lambda owner, half: ref.at[n // 2, c, pl.ds(n % 2 * H + half * Q, Q), place(owner, B)]

    def hidden_of(ref, n):
        return lambda owner, half: ref.at[owner, n // 2, c, pl.ds(n % 2 * H + half * Q, Q)]

    def span(n):
        return pl.ds(n % 2 * H, H)

    def quarters(n):
        return [(half, pl.ds(n % 2 * H + half * Q, Q)) for half in range(2)]

    def piece(m, i, j):
        return w1.at[i, j, c] if m == 1 else w2.at[j, i, c]

    def quarter(m, i):
        return lambda owner, half: piece(m, i, owner).at[pl.ds(half * 64, 64)]

    four = acts.at[0, 0, 0]
    gx = [Gather(net, "y", states_of(xs, n), four) for n in range(CHAINS)]
    others = [lax.rem(x + k, 4) for k in (1, 2, 3)]
    froms = [lax.rem(x + 4 - k, 4) for k in (1, 2, 3)]
    ws, wz, wd = {}, {}, {}
    for m in (1, 2):
        for k, i in enumerate(others):
            src = give1.at[i] if m == 1 else give2.at[:, place(i, B)]
            ws[m, k] = net.copy(src, piece(m, x, z), {"x": i})
        for k, i in enumerate(froms):
            wz[m, k] = Gather(net, "z", quarter(m, i), four)
            slot = net.slots(1)[0]
            for t in range(4):
                mine = piece(m, i, lax.rem(z + t, 4))
                wd[m, k, t] = net.copy(mine, mine, {"c": 1 - c}, slot)
            whole = w1.at[i, :, c] if m == 1 else w2.at[:, i, c]
            wd[m, k] = (whole, whole, {"c": 1 - c}, slot)

    def scatter(axis, k, slots=None):
        return Scatter(net, axis, sent.at[k], far.at[k], near.at[k], held.at[k], slots)

    sh = [scatter("x", n) for n in range(CHAINS)]
    sz = [scatter("y", CHAINS + n) for n in range(CHAINS)]
    sg = [scatter("x", 2 * CHAINS + n, sh[n].slots) for n in range(CHAINS)]
    ga = [Gather(net, "x", hidden_of(acts, n), four) for n in range(CHAINS)]
    gu = [Gather(net, "y", states_of(us, n), four, gx[n].slots) for n in range(CHAINS)]
    gg = [Gather(net, "x", hidden_of(ghs, n), four, ga[n].slots) for n in range(CHAINS)]
    over_y, over_x = net.slots(2)
    ty = [net.copy(totals.at[0, y], totals.at[0, y], {"y": lax.rem(y + k, 4)}, over_y) for k in (1, 2, 3)]
    tx = [net.copy(totals.at[1, x], totals.at[1, x], {"x": lax.rem(x + k, 4)}, over_x) for k in (1, 2, 3)]
    three = totals.at[0, pl.ds(0, 3)]
    ty_all, tx_all = (three, three, partner, over_y), (three, three, partner, over_x)
    def to_partner(ref):
        return net.copy(ref, ref, partner)

    def pair_to_partner(ref, n):
        slot = net.slots(1)[0]
        pair = [ref.at[2 * (1 - c) + e, n // 2, c, span(n)] for e in range(2)]
        both = ref.at[pl.ds(2 * c, 2), n // 2, 1 - c, span(n)]
        return [(p, p, partner, slot) for p in pair], (both, both, partner, slot)

    dx = [[to_partner(xs.at[n // 2, c, span(n)])] for n in range(CHAINS)]
    du = [[to_partner(us.at[n // 2, c, span(n)])] for n in range(CHAINS)]
    da = [pair_to_partner(acts, n) for n in range(CHAINS)]
    dg = [pair_to_partner(ghs, n) for n in range(CHAINS)]
    dr = to_partner(resrow.at[c])
    zs = [
        [Scatter(net, "z", zsent.at[g, r], zfar.at[g, r], znear.at[g, r], zheld.at[g, r]) for r in range(2)] for g in range(2)
    ]

    def per_path(t):
        return jnp.sum(t.T, axis=0, keepdims=True)

    with jax.named_scope("barrier"):
        pl.semaphore_wait(barrier, len(peers))
    gift1.wait()
    for k in (1, 0, 2):
        net.start(ws[1, k])
    fetch[0].wait()
    state = start[...]
    for n in range(STEPS):
        xs[n, c, :, place(y, B)] = state.astype(bf16)
        gx[2 * n].start()
        gx[2 * n + 1].start()
        if n == 0:
            gift2.wait()
            for k in (1, 0, 2):
                net.start(ws[2, k])
        fetch[1 + n].wait()
        state = state + noise_coef * inc[n]
    norm = state * state
    nrow[...] = per_path(norm[:, :128] + norm[:, 128:])
    scalar.wait()

    def put_both(scatter_sum, k, part):
        for half in range(2):
            scatter_sum.put(k, half, part[half * Q : half * Q + Q])

    ready = set()

    def share(key, copies):
        if key not in ready:
            ready.add(key)
            for copy in copies:
                net.start(copy)

    def wait_once(copies):
        for copy in copies:
            if id(copy) not in ready:
                ready.add(id(copy))
                copy.wait()

    def weights(m, k):
        net.arrived(wd[m, k])

    def first(n, k):
        gx[n].finish()
        if k:
            weights(1, 3 - k)
        else:
            wait_once(own1)
        w = w1[lax.rem(x + k, 4)].reshape(4 * B, B)
        put_both(sh[n], k, dot(xs[n // 2, c, span(n)], w, ((1,), (0,))))
        share(("x", n), dx[n])

    def second(n, k):
        ga[n].finish()
        for e in range(3):
            weights(2, e)
        wait_once(own2)
        j = lax.rem(y + k, 4)
        part = None
        for i in range(4):
            term = dot(acts[i, n // 2, c, span(n)], w2[j, i].reshape(B, B), ((1,), (0,)))
            part = term if part is None else part + term
        put_both(sz[n], k, part)
        share(("a", n), da[n][0])

    def third(n, k):
        gu[n].finish()
        i = lax.rem(x + k, 4)
        part = None
        for j in range(4):
            term = dot(us[n // 2, c, span(n), pl.ds(j * B, B)], w2[j, i].reshape(B, B), ((1,), (1,)))
            part = term if part is None else part + term
        put_both(sg[n], k, part)
        share(("u", n), du[n])

    def activate(n):
        for (half, at), h in zip(quarters(n), sh[n].finish()):
            sig = jax.nn.sigmoid(h)
            acts[x, n // 2, c, at] = (h * sig).astype(bf16)
            slopes[n, half] = sig * (1.0 + h * (1.0 - sig))
        ga[n].start()

    begun = set()

    def control(n):
        for (half, at), total in zip(quarters(n), sz[n].finish()):
            zval = zscale * total
            dw = inc[n // 2, at, :]
            us[n // 2, c, at, place(y, B)] = (zscale * (lam_coef * time_step * zval + dw)).astype(bf16)
            term = 0.5 * lam_coef * time_step * zval * zval + zval * dw
            term = term[:, :128] + term[:, 128:]
            folded[at, :] = folded[at, :] + term if n % 2 in begun else term
        begun.add(n % 2)
        gu[n].start()

    def hidden_grad(n):
        for (half, at), g in zip(quarters(n), sg[n].finish()):
            r = rowres[c, at, :]
            r = jnp.concatenate([r, r], axis=1)
            ghs[x, n // 2, c, at] = (r * g * slopes[n, half]).astype(bf16)
        gg[n].start()

    def totals_y():
        y_row = per_path(folded[...])
        totals[0, y] = jnp.concatenate([y_row, nrow[...], jnp.zeros((6, B), f32)], axis=0)
        for copy in ty:
            net.start(copy)

    def totals_x():
        net.arrived(ty_all)
        totals[1, x] = totals[0, 0] + totals[0, 1] + totals[0, 2] + totals[0, 3]
        for copy in tx:
            net.start(copy)

    kept_row = pltpu.make_async_copy(resrow.at[c], res_out, local.at[12])

    def residuals():
        net.arrived(tx_all)
        both = totals[1, 0] + totals[1, 1] + totals[1, 2] + totals[1, 3]
        residual = initial[0] + both[0:1] - jnp.log((1.0 + both[1:2]) * 0.5)
        resrow[c] = jnp.broadcast_to(residual, (8, B))
        net.start(dr)
        kept_row.start()
        rowres[c] = jnp.broadcast_to(residual, (128, B)).T

    def partner_residuals():
        net.arrived(dr)
        rowres[1 - c] = jnp.broadcast_to(resrow[1 - c, 0:1], (128, B)).T

    def scale(n):
        net.arrived(da[n][1])
        for e in range(2):
            for core in range(2):
                for k in range(2):
                    lanes = pl.ds(k * 128, 128)
                    a = acts[2 * c + e, n // 2, core, span(n), lanes].astype(f32)
                    scaled[e, n // 2, core, span(n), lanes] = (a * rowres[core, span(n)]).astype(bf16)

    def out_sum(e):
        for n in range(CHAINS):
            gu[n].finish()
            for copy in du[n]:
                net.arrived(copy)
        every = STEPS * 2 * B
        acc[1, e] = dot(scaled[e].reshape(every, B), us[...].reshape(every, 4 * B), ((0,), (0,)))

    def give(n):
        gg[n].finish()
        for copy in dg[n][0]:
            net.start(copy)

    def of_chain(e, n):
        for copy in dx[n] + [dg[n][1]]:
            net.arrived(copy)
        g = ghs[2 * c + e, n // 2, :, span(n)].reshape(B, B)
        return dot(g, xs[n // 2, :, span(n)].reshape(B, 4 * B), ((0,), (0,)))

    def in_sum(e):
        for n in range(4):
            for copy in dx[n] + [dg[n][1]]:
                net.arrived(copy)
        g = ghs[2 * c + e, pl.ds(0, 2)].reshape(4 * B, B)
        acc[0, e] = dot(g, xs[pl.ds(0, 2)].reshape(4 * B, 4 * B), ((0,), (0,))) + of_chain(e, 4)

    def in_last(e):
        acc[0, e] = acc[0, e] + of_chain(e, 5)

    def over_z(g, r, k):
        cols = place(lax.rem(z + k, 4), B)
        for e in range(2):
            zs[g][r].put(k, e, acc[g, e, pl.ds(r * H, H), cols])

    def leaving(g, r, e, slot):
        rows = pl.ds(r * H, H)
        k = 4 * g + 2 * r
        return pltpu.make_async_remote_copy(
            src_ref=leave.at[g, e, rows],
            dst_ref=grads_out.at[g, slot, rows],
            send_sem=send.at[LEAVING + k + e],
            recv_sem=recv.at[ARRIVALS + k + slot],
            device_id={"x": 2 * c + e, "c": x // 2},
            device_id_type=MESH,
        )

    def staying(g, r, e):
        rows = pl.ds(r * H, H)
        return pltpu.make_async_copy(leave.at[g, e, rows], grads_out.at[g, e, rows], local.at[13 + 4 * g + 2 * r + e])

    def to_owner(g, r):
        for e, value in enumerate(zs[g][r].finish()):
            leave[g, e, pl.ds(r * H, H)] = value.astype(bf16)

            @pl.when(2 * c + e != x)
            def _(e=e):
                leaving(g, r, e, lax.rem(x, 2)).start()

            @pl.when(2 * c + e == x)
            def _(e=e):
                staying(g, r, e).start()

    def collect(g):
        for r in range(2):
            for e in range(2):

                @pl.when(2 * c + e != x)
                def _(r=r, e=e):
                    copy = leaving(g, r, e, e)
                    copy.wait_recv()
                    copy.wait_send()

                @pl.when(2 * c + e == x)
                def _(r=r, e=e):
                    staying(g, r, e).wait()

    def weights_in(m, k):
        net.arrived(ws[m, k])
        wz[m, k].start()
        net.start(wd[m, k, 0])

    def weights_out(m, k):
        wz[m, k].finish()
        for t in (1, 3, 2):
            net.start(wd[m, k, t])

    tasks = {"tot": totals_y, "tot2": totals_x, "res": residuals, "resp": partner_residuals}
    for m in (1, 2):
        for k in range(3):
            tasks[f"w{m}a{k}"] = lambda m=m, k=k: weights_in(m, k)
            tasks[f"w{m}b{k}"] = wz[m, k].mid
            tasks[f"w{m}c{k}"] = lambda m=m, k=k: weights_out(m, k)
    for n in range(CHAINS):
        for k in range(4):
            tasks[f"f{n}{k}"] = lambda n=n, k=k: first(n, k)
            tasks[f"s{n}{k}"] = lambda n=n, k=k: second(n, k)
            tasks[f"t{n}{k}"] = lambda n=n, k=k: third(n, k)
        named = {"gx": gx, "sh": sh, "ga": ga, "sz": sz, "gu": gu, "sg": sg, "gg": gg}
        for name, ops in named.items():
            tasks[f"{name}{n}.mid"] = ops[n].mid
        tasks[f"act{n}"] = lambda n=n: activate(n)
        tasks[f"con{n}"] = lambda n=n: control(n)
        tasks[f"hid{n}"] = lambda n=n: hidden_grad(n)
        tasks[f"sc{n}"] = lambda n=n: scale(n)
        tasks[f"gs{n}"] = lambda n=n: give(n)

    for e in range(2):
        tasks[f"go{e}"] = lambda e=e: out_sum(e)
        tasks[f"gi{e}"] = lambda e=e: in_sum(e)
        tasks[f"gj{e}"] = lambda e=e: in_last(e)
    for g, name in enumerate("io"):
        for r in range(2):
            for k in range(4):
                tasks[f"p{name}{r}{k}"] = lambda g=g, r=r, k=k: over_z(g, r, k)
            tasks[f"z{name}{r}.mid"] = zs[g][r].mid
            tasks[f"z{name}{r}.fin"] = lambda g=g, r=r: to_owner(g, r)
        tasks[f"col{name}"] = lambda g=g: collect(g)

    assert sorted(PROGRAM) == sorted(tasks)
    for name in PROGRAM:
        with jax.named_scope(name):
            tasks[name]()
    kept_row.wait()
    net.drain()


def placing(row, blocks, residual, grad_in, grad_out):
    residual[...] = row[0:1].reshape(B)
    for t in range(2):
        grad_in[pl.ds(t * B, B), :] = blocks[0, t].astype(f32).T
        grad_out[:, pl.ds(t * B, B)] = blocks[1, t].astype(f32)


def on_device(start, increments, w_in, w_out, initial):
    vmem, anywhere = pl.BlockSpec(memory_space=pltpu.VMEM), pl.BlockSpec(memory_space=pl.ANY)
    states = pltpu.VMEM((STEPS, 2, B, 4 * B), bf16)
    hidden = pltpu.VMEM((4, STEPS, 2, B, B), bf16)
    weights = pltpu.VMEM((4, 4, 2, H, B), bf16)
    row, blocks = pl.pallas_call(
        kernel,
        out_shape=(jax.ShapeDtypeStruct((8, B), f32), jax.ShapeDtypeStruct((2, 2, B, B), bf16)),
        in_specs=[anywhere] * 5,
        out_specs=(anywhere, anywhere),
        scratch_shapes=[
            pltpu.VMEM((B, B), f32),
            pltpu.VMEM((STEPS, B, B), f32),
            states,
            states,
            hidden,
            pltpu.VMEM((2, STEPS, 2, B, B), bf16),
            hidden,
            weights,
            weights,
            pltpu.VMEM((CHAINS, 2, Q, B), f32),
            pltpu.VMEM((3 * CHAINS, 3, 2, Q, B), bf16),
            pltpu.VMEM((3 * CHAINS, 2, Q, B), bf16),
            pltpu.VMEM((3 * CHAINS, 2, 2, Q, B), bf16),
            pltpu.VMEM((3 * CHAINS, 4, Q, B), f32),
            pltpu.VMEM((2, 2, B, 4 * B), f32),
            pltpu.VMEM((2, 2, 3, 2, H, B), bf16),
            pltpu.VMEM((2, 2, 2, H, B), bf16),
            pltpu.VMEM((2, 2, 4, H, B), f32),
            pltpu.VMEM((2, 2, 2, 2, H, B), bf16),
            pltpu.VMEM((2, 2, B, B), bf16),
            pltpu.VMEM((2, 4, 8, B), f32),
            pltpu.VMEM((1, B), f32),
            pltpu.VMEM((B, 128), f32),
            pltpu.VMEM((2, 8, B), f32),
            pltpu.VMEM((2, B, 128), f32),
            pltpu.VMEM((4, H, B), bf16),
            pltpu.VMEM((H, 4 * B), bf16),
            pltpu.SMEM((1,), f32),
            pltpu.SemaphoreType.DMA((LEAVING + 8,)),
            pltpu.SemaphoreType.DMA((ARRIVALS + 8,)),
            pltpu.SemaphoreType.DMA((21,)),
        ],
        compiler_params=pltpu.CompilerParams(collective_id=0, has_side_effects=True, vmem_limit_bytes=66000000),
    )(start, increments, w_in.reshape(4, 4, 2, H, B), w_out.reshape(2, H, D), initial.reshape(1))
    return pl.pallas_call(
        placing,
        out_shape=(
            jax.ShapeDtypeStruct((B,), f32),
            jax.ShapeDtypeStruct((2 * B, B), f32),
            jax.ShapeDtypeStruct((B, 2 * B), f32),
        ),
        in_specs=[vmem, vmem],
        out_specs=(vmem, vmem, vmem),
    )(row, blocks)


def solution(mesh):
    finer = Mesh(mesh.devices.reshape(4, 4, 4, 2), ("y", "x", "z", "c"))
    return jax.shard_map(
        on_device,
        mesh=finer,
        in_specs=(P(BATCH, DIM), P(None, BATCH, DIM), P(None, DIM), P(DIM, None), P()),
        out_specs=(P(BATCH), P(BATCH, DIM), P(DIM, BATCH)),
        check_vma=False,
    )
```

```python
import math

import jax
import jax.numpy as jnp
from jax import lax
from jax.experimental import pallas as pl
from jax.experimental.pallas import tpu as pltpu
from jax.sharding import Mesh
from jax.sharding import PartitionSpec as P

D = 4096
STEPS = 3
B = 256
H = B // 2
Q = B // 4
CHAINS = 2 * STEPS
DIM = ("y", "x")
BATCH = ("z", "c")
MESH = pl.DeviceIdType.MESH
f32, bf16 = jnp.float32, jnp.bfloat16

time_step = 1.0 / 64.0
lam_coef = 50.0
noise_coef = math.sqrt(2.0)
zscale = 2.0 / math.sqrt(D)
ARRIVALS = 170
LEAVING = 48


def place(pos, extent):
    return pl.ds(pl.multiple_of(pos * extent, extent), extent)


class Net:

    def __init__(self, send, recv):
        self.send, self.recv, self.count, self.begun, self.seen = send, recv, 0, [], set()

    def slots(self, count):
        self.count += count
        assert self.count <= ARRIVALS
        return [self.recv.at[k] for k in range(self.count - count, self.count)]

    def copy(self, src, dst, device, slot=None):
        return (src, dst, device, self.slots(1)[0] if slot is None else slot)

    def made(self, copy, send):
        src, dst, device, slot = copy
        return pltpu.make_async_remote_copy(
            src_ref=src, dst_ref=dst, send_sem=send, recv_sem=slot, device_id=device, device_id_type=MESH
        )

    def start(self, copy):
        send = self.send.at[len(self.begun) % LEAVING]
        if len(self.begun) >= LEAVING:
            self.begun[len(self.begun) - LEAVING].wait_send()
        made = self.made(copy, send)
        made.start()
        self.begun.append(made)

    def arrived(self, copy):
        if id(copy) not in self.seen:
            self.seen.add(id(copy))
            self.made(copy, self.send.at[0]).wait_recv()

    def drain(self):
        for copy in self.begun[-LEAVING:]:
            copy.wait_send()


class Gather:

    def __init__(self, net, axis, view, four, slots=None):
        p = lax.axis_index(axis)
        r, l = lax.rem(p + 1, 4), lax.rem(p + 3, 4)
        self.net, self.slots = net, slots or net.slots(3)
        self.copies = [
            net.copy(view(owner, half), view(owner, half), {axis: to}, self.slots[min(k, 2)])
            for k, (owner, half, to) in enumerate(((p, 0, r), (p, 1, l), (p, 1, r), (p, 0, l), (l, 0, r), (r, 1, l)))
        ]
        self.rest = (four, four, {axis: r}, self.slots[2])

    def start(self):
        for k in range(4):
            self.net.start(self.copies[k])

    def mid(self):
        for k in range(2):
            self.net.arrived(self.copies[k])
            self.net.start(self.copies[4 + k])

    def finish(self):
        self.net.arrived(self.rest)


class Scatter:

    def __init__(self, net, axis, sent, far, near, held, slots=None):
        p = lax.axis_index(axis)
        r, l = {axis: lax.rem(p + 1, 4)}, {axis: lax.rem(p + 3, 4)}
        self.net, self.sent, self.far, self.near, self.held = net, sent, far, near, held
        self.slots = slots or net.slots(3)
        a, b, rest = self.slots
        self.copies = {
            (2, 0): net.copy(sent.at[1, 0], far.at[0], r, a),
            (2, 1): net.copy(sent.at[1, 1], far.at[1], l, b),
            (1, 1): net.copy(sent.at[0, 1], near.at[0, 1], r, rest),
            (3, 0): net.copy(sent.at[2, 0], near.at[1, 0], l, rest),
            (1, 0): net.copy(sent.at[0, 0], near.at[0, 0], r, rest),
            (3, 1): net.copy(sent.at[2, 1], near.at[1, 1], l, rest),
        }
        self.rest = (near, near, r, rest)

    def put(self, k, half, value):
        if (k, half) in ((2, 0), (2, 1), (1, 1), (3, 0)):
            self.sent[k - 1, half] = value.astype(bf16)
            self.net.start(self.copies[k, half])
        else:
            self.held[{0: half, 1: 2, 3: 3}[k]] = value

    def mid(self):
        for side, key in enumerate(((1, 0), (3, 1))):
            self.net.arrived(self.copies[2, side])
            k, half = key
            self.sent[k - 1, half] = (self.held[2 + side] + self.far[side].astype(f32)).astype(bf16)
            self.net.start(self.copies[key])

    def finish(self):
        self.net.arrived(self.rest)
        near = self.near
        return [self.held[half] + near[0, half].astype(f32) + near[1, half].astype(f32) for half in range(2)]


ORDER = (2, 1, 3, 0)
PROGRAM = [
    "w1a2", "w1a1", "w1a0", "w1b2", "gx3.mid", "w1b1", "gx4.mid", "w1b0", "w1c2", "gx2.mid", "gx5.mid", "w2a0",
    "w1c1", "f32", "w2a2", "w2a1", "f42", "w1c0", "f22", "f52", "f21", "f23", "w2b0", "f43", "gx0.mid", "f41",
    "gx1.mid", "f30", "sh4.mid", "sh2.mid", "w2b2", "f40", "f53", "f51", "sh5.mid", "w2c0", "w2b1", "f31", "f33",
    "act4", "w2c2", "f00", "f50", "f20", "act2", "w2c1", "ga4.mid", "act5", "ga2.mid", "f12", "sh3.mid", "s42", "s43",
    "f02", "s41", "ga5.mid", "f11", "f13", "s22", "sh1.mid", "s21", "s23", "sz4.mid", "act3", "f03", "f01", "s20",
    "sh0.mid", "s52", "f10", "sz2.mid", "s51", "s53", "act1", "s40", "con4", "s50", "ga3.mid", "sz5.mid", "act0",
    "con2", "gu4.mid", "ga1.mid", "s33", "s31", "s32", "ga0.mid", "s30", "con5", "gu2.mid", "s12", "t42", "s02",
    "gu5.mid", "s01", "s00", "s03", "t43", "sz3.mid", "s11", "s13", "s10", "sz1.mid", "t21", "sz0.mid", "t53", "t40",
    "t52", "t22", "con3", "t51", "con1", "t23", "t41", "con0", "sg4.mid", "t20", "tot", "sg5.mid", "gu3.mid", "t50",
    "sg2.mid", "gu1.mid", "gu0.mid", "tot2", "t32", "t33", "t31", "t12", "t11", "t13", "t02", "t01", "sg3.mid", "res",
    "hid5", "t03", "t10", "hid2", "sg0.mid", "sg1.mid", "resp", "sc1", "sc3", "sc4", "sc2", "sc0", "sc5", "hid4",
    "gg5.mid", "go0", "t30", "go1", "po10", "hid3", "po02", "t00", "po03", "po01", "po12", "hid0", "hid1", "gg4.mid",
    "po00", "zo0.mid", "po13", "gg2.mid", "gg3.mid", "gg0.mid", "po11", "gg1.mid", "zo1.mid", "gs2", "gs3", "gs4",
    "gs5", "gs0", "gs1", "gi1", "gi0", "gj1", "gj0", "pi12", "pi13", "pi11", "zo0.fin", "pi02", "zo1.fin", "pi10",
    "zi1.mid", "pi03", "pi01", "zi0.mid", "zi1.fin", "colo", "pi00", "zi0.fin", "coli",
]


def dot(a, b, dims):
    return lax.dot_general(a, b, (dims, ((), ())), preferred_element_type=f32)


def kernel(
    start_in, inc_in, w_in, w_out, initial_in,
    res_out, grads_out,
    start, inc, xs, us, acts, scaled, ghs, w1, w2, slopes,
    sent, far, near, held, acc, zsent, zfar, zheld, znear,
    leave, totals, nrow, folded, resrow, rowres, give1, give2, initial, send, recv, local,
):
    y, x, z, c = (lax.axis_index(a) for a in ("y", "x", "z", "c"))

    barrier = pltpu.get_barrier_semaphore()
    peers = [{a: lax.rem(i + k, 4)} for a, i in (("x", x), ("y", y)) for k in (1, 2, 3)]
    peers += [{"z": lax.rem(z + k, 4)} for k in (1, 3)]
    peers += [{"c": 1 - c}] + [{"x": lax.rem(x + k, 4), "c": 1 - c} for k in (1, 2, 3)]
    for peer in peers:
        pl.semaphore_signal(barrier, inc=1, device_id=peer, device_id_type=MESH)

    fetch = [pltpu.make_async_copy(start_in, start, local.at[0])]
    fetch += [pltpu.make_async_copy(inc_in.at[n], inc.at[n], local.at[1 + n]) for n in range(STEPS)]
    own1 = [pltpu.make_async_copy(w_in.at[:, x], w1.at[x], local.at[4])]
    own2 = []
    for j in range(4):
        cols = pl.ds(pl.multiple_of(1024 * j + x * B, B), B)
        own2.append(pltpu.make_async_copy(w_out.at[:, :, cols], w2.at[j, x], local.at[5 + j]))
    gift1 = pltpu.make_async_copy(w_in.at[z, :, c], give1, local.at[9])
    gift2 = pltpu.make_async_copy(w_out.at[c, :, pl.ds(pl.multiple_of(z * 1024, 1024), 1024)], give2, local.at[10])
    scalar = pltpu.make_async_copy(initial_in, initial, local.at[11])
    for copy in [gift1] + fetch + [gift2] + own1 + own2 + [scalar]:
        copy.start()

    net = Net(send, recv)
    partner = {"c": 1 - c}

    def states_of(ref, n):
        return lambda owner, half: ref.at[n // 2, c, pl.ds(n % 2 * H + half * Q, Q), place(owner, B)]

    def hidden_of(ref, n):
        return lambda owner, half: ref.at[owner, n // 2, c, pl.ds(n % 2 * H + half * Q, Q)]

    def span(n):
        return pl.ds(n % 2 * H, H)

    def quarters(n):
        return [(half, pl.ds(n % 2 * H + half * Q, Q)) for half in range(2)]

    def piece(m, i, j):
        return w1.at[i, j, c] if m == 1 else w2.at[j, i, c]

    def quarter(m, i):
        return lambda owner, half: piece(m, i, owner).at[pl.ds(half * 64, 64)]

    four = acts.at[0, 0, 0]
    gx = [Gather(net, "y", states_of(xs, n), four) for n in range(CHAINS)]
    others = [lax.rem(x + k, 4) for k in (1, 2, 3)]
    froms = [lax.rem(x + 4 - k, 4) for k in (1, 2, 3)]
    ws, wz, wd = {}, {}, {}
    for m in (1, 2):
        for k, i in enumerate(others):
            src = give1.at[i] if m == 1 else give2.at[:, place(i, B)]
            ws[m, k] = net.copy(src, piece(m, x, z), {"x": i})
        for k, i in enumerate(froms):
            wz[m, k] = Gather(net, "z", quarter(m, i), four)
            slot = net.slots(1)[0]
            for t in range(4):
                mine = piece(m, i, lax.rem(z + t, 4))
                wd[m, k, t] = net.copy(mine, mine, {"c": 1 - c}, slot)
            whole = w1.at[i, :, c] if m == 1 else w2.at[:, i, c]
            wd[m, k] = (whole, whole, {"c": 1 - c}, slot)

    def scatter(axis, k, slots=None):
        return Scatter(net, axis, sent.at[k], far.at[k], near.at[k], held.at[k], slots)

    sh = [scatter("x", n) for n in range(CHAINS)]
    sz = [scatter("y", CHAINS + n) for n in range(CHAINS)]
    sg = [scatter("x", 2 * CHAINS + n, sh[n].slots) for n in range(CHAINS)]
    ga = [Gather(net, "x", hidden_of(acts, n), four) for n in range(CHAINS)]
    gu = [Gather(net, "y", states_of(us, n), four, gx[n].slots) for n in range(CHAINS)]
    gg = [Gather(net, "x", hidden_of(ghs, n), four, ga[n].slots) for n in range(CHAINS)]
    over_y, over_x = net.slots(2)
    ty = [net.copy(totals.at[0, y], totals.at[0, y], {"y": lax.rem(y + k, 4)}, over_y) for k in (1, 2, 3)]
    tx = [net.copy(totals.at[1, x], totals.at[1, x], {"x": lax.rem(x + k, 4)}, over_x) for k in (1, 2, 3)]
    three = totals.at[0, pl.ds(0, 3)]
    ty_all, tx_all = (three, three, partner, over_y), (three, three, partner, over_x)
    def to_partner(ref):
        return net.copy(ref, ref, partner)

    def pair_to_partner(ref, n):
        slot = net.slots(1)[0]
        pair = [ref.at[2 * (1 - c) + e, n // 2, c, span(n)] for e in range(2)]
        both = ref.at[pl.ds(2 * c, 2), n // 2, 1 - c, span(n)]
        return [(p, p, partner, slot) for p in pair], (both, both, partner, slot)

    dx = [[to_partner(xs.at[n // 2, c, span(n)])] for n in range(CHAINS)]
    du = [[to_partner(us.at[n // 2, c, span(n)])] for n in range(CHAINS)]
    da = [pair_to_partner(acts, n) for n in range(CHAINS)]
    dg = [pair_to_partner(ghs, n) for n in range(CHAINS)]
    dr = to_partner(resrow.at[c])
    zs = [
        [Scatter(net, "z", zsent.at[g, r], zfar.at[g, r], znear.at[g, r], zheld.at[g, r]) for r in range(2)] for g in range(2)
    ]

    def per_path(t):
        return jnp.sum(t.T, axis=0, keepdims=True)

    with jax.named_scope("barrier"):
        pl.semaphore_wait(barrier, len(peers))
    gift1.wait()
    for k in (1, 0, 2):
        net.start(ws[1, k])
    fetch[0].wait()
    state = start[...]
    for n in range(STEPS):
        xs[n, c, :, place(y, B)] = state.astype(bf16)
        gx[2 * n].start()
        gx[2 * n + 1].start()
        if n == 0:
            gift2.wait()
            for k in (1, 0, 2):
                net.start(ws[2, k])
        fetch[1 + n].wait()
        state = state + noise_coef * inc[n]
    norm = state * state
    nrow[...] = per_path(norm[:, :128] + norm[:, 128:])
    scalar.wait()

    def put_both(scatter_sum, k, part):
        for half in range(2):
            scatter_sum.put(k, half, part[half * Q : half * Q + Q])

    ready = set()

    def share(key, copies):
        if key not in ready:
            ready.add(key)
            for copy in copies:
                net.start(copy)

    def wait_once(copies):
        for copy in copies:
            if id(copy) not in ready:
                ready.add(id(copy))
                copy.wait()

    def weights(m, k):
        net.arrived(wd[m, k])

    def first(n, k):
        gx[n].finish()
        if k:
            weights(1, 3 - k)
        else:
            wait_once(own1)
        w = w1[lax.rem(x + k, 4)].reshape(4 * B, B)
        put_both(sh[n], k, dot(xs[n // 2, c, span(n)], w, ((1,), (0,))))
        share(("x", n), dx[n])

    def second(n, k):
        ga[n].finish()
        for e in range(3):
            weights(2, e)
        wait_once(own2)
        j = lax.rem(y + k, 4)
        part = None
        for i in range(4):
            term = dot(acts[i, n // 2, c, span(n)], w2[j, i].reshape(B, B), ((1,), (0,)))
            part = term if part is None else part + term
        put_both(sz[n], k, part)
        share(("a", n), da[n][0])

    def third(n, k):
        gu[n].finish()
        i = lax.rem(x + k, 4)
        part = None
        for j in range(4):
            term = dot(us[n // 2, c, span(n), pl.ds(j * B, B)], w2[j, i].reshape(B, B), ((1,), (1,)))
            part = term if part is None else part + term
        put_both(sg[n], k, part)
        share(("u", n), du[n])

    def activate(n):
        for (half, at), h in zip(quarters(n), sh[n].finish()):
            sig = jax.nn.sigmoid(h)
            acts[x, n // 2, c, at] = (h * sig).astype(bf16)
            slopes[n, half] = sig * (1.0 + h * (1.0 - sig))
        ga[n].start()

    begun = set()

    def control(n):
        for (half, at), total in zip(quarters(n), sz[n].finish()):
            zval = zscale * total
            dw = inc[n // 2, at, :]
            us[n // 2, c, at, place(y, B)] = (zscale * (lam_coef * time_step * zval + dw)).astype(bf16)
            term = 0.5 * lam_coef * time_step * zval * zval + zval * dw
            term = term[:, :128] + term[:, 128:]
            folded[at, :] = folded[at, :] + term if n % 2 in begun else term
        begun.add(n % 2)
        gu[n].start()

    def hidden_grad(n):
        for (half, at), g in zip(quarters(n), sg[n].finish()):
            r = rowres[c, at, :]
            r = jnp.concatenate([r, r], axis=1)
            ghs[x, n // 2, c, at] = (r * g * slopes[n, half]).astype(bf16)
        gg[n].start()

    def totals_y():
        y_row = per_path(folded[...])
        totals[0, y] = jnp.concatenate([y_row, nrow[...], jnp.zeros((6, B), f32)], axis=0)
        for copy in ty:
            net.start(copy)

    def totals_x():
        net.arrived(ty_all)
        totals[1, x] = totals[0, 0] + totals[0, 1] + totals[0, 2] + totals[0, 3]
        for copy in tx:
            net.start(copy)

    kept_row = pltpu.make_async_copy(resrow.at[c], res_out, local.at[12])

    def residuals():
        net.arrived(tx_all)
        both = totals[1, 0] + totals[1, 1] + totals[1, 2] + totals[1, 3]
        residual = initial[0] + both[0:1] - jnp.log((1.0 + both[1:2]) * 0.5)
        resrow[c] = jnp.broadcast_to(residual, (8, B))
        net.start(dr)
        kept_row.start()
        rowres[c] = jnp.broadcast_to(residual, (128, B)).T

    def partner_residuals():
        net.arrived(dr)
        rowres[1 - c] = jnp.broadcast_to(resrow[1 - c, 0:1], (128, B)).T

    def scale(n):
        net.arrived(da[n][1])
        for e in range(2):
            for core in range(2):
                for k in range(2):
                    lanes = pl.ds(k * 128, 128)
                    a = acts[2 * c + e, n // 2, core, span(n), lanes].astype(f32)
                    scaled[e, n // 2, core, span(n), lanes] = (a * rowres[core, span(n)]).astype(bf16)

    def out_sum(e):
        for n in range(CHAINS):
            gu[n].finish()
            for copy in du[n]:
                net.arrived(copy)
        every = STEPS * 2 * B
        acc[1, e] = dot(scaled[e].reshape(every, B), us[...].reshape(every, 4 * B), ((0,), (0,)))

    def give(n):
        gg[n].finish()
        for copy in dg[n][0]:
            net.start(copy)

    def of_chain(e, n):
        for copy in dx[n] + [dg[n][1]]:
            net.arrived(copy)
        g = ghs[2 * c + e, n // 2, :, span(n)].reshape(B, B)
        return dot(g, xs[n // 2, :, span(n)].reshape(B, 4 * B), ((0,), (0,)))

    def in_sum(e):
        for n in range(4):
            for copy in dx[n] + [dg[n][1]]:
                net.arrived(copy)
        g = ghs[2 * c + e, pl.ds(0, 2)].reshape(4 * B, B)
        acc[0, e] = dot(g, xs[pl.ds(0, 2)].reshape(4 * B, 4 * B), ((0,), (0,))) + of_chain(e, 4)

    def in_last(e):
        acc[0, e] = acc[0, e] + of_chain(e, 5)

    def over_z(g, r, k):
        cols = place(lax.rem(z + k, 4), B)
        for e in range(2):
            zs[g][r].put(k, e, acc[g, e, pl.ds(r * H, H), cols])

    def leaving(g, r, e, slot):
        rows = pl.ds(r * H, H)
        k = 4 * g + 2 * r
        return pltpu.make_async_remote_copy(
            src_ref=leave.at[g, e, rows],
            dst_ref=grads_out.at[g, slot, rows],
            send_sem=send.at[LEAVING + k + e],
            recv_sem=recv.at[ARRIVALS + k + slot],
            device_id={"x": 2 * c + e, "c": x // 2},
            device_id_type=MESH,
        )

    def staying(g, r, e):
        rows = pl.ds(r * H, H)
        return pltpu.make_async_copy(leave.at[g, e, rows], grads_out.at[g, e, rows], local.at[13 + 4 * g + 2 * r + e])

    def to_owner(g, r):
        for e, value in enumerate(zs[g][r].finish()):
            leave[g, e, pl.ds(r * H, H)] = value.astype(bf16)

            @pl.when(2 * c + e != x)
            def _(e=e):
                leaving(g, r, e, lax.rem(x, 2)).start()

            @pl.when(2 * c + e == x)
            def _(e=e):
                staying(g, r, e).start()

    def collect(g):
        for r in range(2):
            for e in range(2):

                @pl.when(2 * c + e != x)
                def _(r=r, e=e):
                    copy = leaving(g, r, e, e)
                    copy.wait_recv()
                    copy.wait_send()

                @pl.when(2 * c + e == x)
                def _(r=r, e=e):
                    staying(g, r, e).wait()

    def weights_in(m, k):
        net.arrived(ws[m, k])
        wz[m, k].start()
        net.start(wd[m, k, 0])

    def weights_out(m, k):
        wz[m, k].finish()
        for t in (1, 3, 2):
            net.start(wd[m, k, t])

    tasks = {"tot": totals_y, "tot2": totals_x, "res": residuals, "resp": partner_residuals}
    for m in (1, 2):
        for k in range(3):
            tasks[f"w{m}a{k}"] = lambda m=m, k=k: weights_in(m, k)
            tasks[f"w{m}b{k}"] = wz[m, k].mid
            tasks[f"w{m}c{k}"] = lambda m=m, k=k: weights_out(m, k)
    for n in range(CHAINS):
        for k in range(4):
            tasks[f"f{n}{k}"] = lambda n=n, k=k: first(n, k)
            tasks[f"s{n}{k}"] = lambda n=n, k=k: second(n, k)
            tasks[f"t{n}{k}"] = lambda n=n, k=k: third(n, k)
        named = {"gx": gx, "sh": sh, "ga": ga, "sz": sz, "gu": gu, "sg": sg, "gg": gg}
        for name, ops in named.items():
            tasks[f"{name}{n}.mid"] = ops[n].mid
        tasks[f"act{n}"] = lambda n=n: activate(n)
        tasks[f"con{n}"] = lambda n=n: control(n)
        tasks[f"hid{n}"] = lambda n=n: hidden_grad(n)
        tasks[f"sc{n}"] = lambda n=n: scale(n)
        tasks[f"gs{n}"] = lambda n=n: give(n)

    for e in range(2):
        tasks[f"go{e}"] = lambda e=e: out_sum(e)
        tasks[f"gi{e}"] = lambda e=e: in_sum(e)
        tasks[f"gj{e}"] = lambda e=e: in_last(e)
    for g, name in enumerate("io"):
        for r in range(2):
            for k in range(4):
                tasks[f"p{name}{r}{k}"] = lambda g=g, r=r, k=k: over_z(g, r, k)
            tasks[f"z{name}{r}.mid"] = zs[g][r].mid
            tasks[f"z{name}{r}.fin"] = lambda g=g, r=r: to_owner(g, r)
        tasks[f"col{name}"] = lambda g=g: collect(g)

    assert sorted(PROGRAM) == sorted(tasks)
    for name in PROGRAM:
        with jax.named_scope(name):
            tasks[name]()
    kept_row.wait()
    net.drain()


def placing(row, blocks, residual, grad_in, grad_out):
    residual[...] = row[0:1].reshape(B)
    for t in range(2):
        grad_in[pl.ds(t * B, B), :] = blocks[0, t].astype(f32).T
        grad_out[:, pl.ds(t * B, B)] = blocks[1, t].astype(f32)


def on_device(start, increments, w_in, w_out, initial):
    vmem, anywhere = pl.BlockSpec(memory_space=pltpu.VMEM), pl.BlockSpec(memory_space=pl.ANY)
    states = pltpu.VMEM((STEPS, 2, B, 4 * B), bf16)
    hidden = pltpu.VMEM((4, STEPS, 2, B, B), bf16)
    weights = pltpu.VMEM((4, 4, 2, H, B), bf16)
    row, blocks = pl.pallas_call(
        kernel,
        out_shape=(jax.ShapeDtypeStruct((8, B), f32), jax.ShapeDtypeStruct((2, 2, B, B), bf16)),
        in_specs=[anywhere] * 5,
        out_specs=(anywhere, anywhere),
        scratch_shapes=[
            pltpu.VMEM((B, B), f32),
            pltpu.VMEM((STEPS, B, B), f32),
            states,
            states,
            hidden,
            pltpu.VMEM((2, STEPS, 2, B, B), bf16),
            hidden,
            weights,
            weights,
            pltpu.VMEM((CHAINS, 2, Q, B), f32),
            pltpu.VMEM((3 * CHAINS, 3, 2, Q, B), bf16),
            pltpu.VMEM((3 * CHAINS, 2, Q, B), bf16),
            pltpu.VMEM((3 * CHAINS, 2, 2, Q, B), bf16),
            pltpu.VMEM((3 * CHAINS, 4, Q, B), f32),
            pltpu.VMEM((2, 2, B, 4 * B), f32),
            pltpu.VMEM((2, 2, 3, 2, H, B), bf16),
            pltpu.VMEM((2, 2, 2, H, B), bf16),
            pltpu.VMEM((2, 2, 4, H, B), f32),
            pltpu.VMEM((2, 2, 2, 2, H, B), bf16),
            pltpu.VMEM((2, 2, B, B), bf16),
            pltpu.VMEM((2, 4, 8, B), f32),
            pltpu.VMEM((1, B), f32),
            pltpu.VMEM((B, 128), f32),
            pltpu.VMEM((2, 8, B), f32),
            pltpu.VMEM((2, B, 128), f32),
            pltpu.VMEM((4, H, B), bf16),
            pltpu.VMEM((H, 4 * B), bf16),
            pltpu.SMEM((1,), f32),
            pltpu.SemaphoreType.DMA((LEAVING + 8,)),
            pltpu.SemaphoreType.DMA((ARRIVALS + 8,)),
            pltpu.SemaphoreType.DMA((21,)),
        ],
        compiler_params=pltpu.CompilerParams(collective_id=0, has_side_effects=True, vmem_limit_bytes=66000000),
    )(start, increments, w_in.reshape(4, 4, 2, H, B), w_out.reshape(2, H, D), initial.reshape(1))
    return pl.pallas_call(
        placing,
        out_shape=(
            jax.ShapeDtypeStruct((B,), f32),
            jax.ShapeDtypeStruct((2 * B, B), f32),
            jax.ShapeDtypeStruct((B, 2 * B), f32),
        ),
        in_specs=[vmem, vmem],
        out_specs=(vmem, vmem, vmem),
    )(row, blocks)


def solution(mesh):
    finer = Mesh(mesh.devices.reshape(4, 4, 4, 2), ("y", "x", "z", "c"))
    return jax.shard_map(
        on_device,
        mesh=finer,
        in_specs=(P(BATCH, DIM), P(None, BATCH, DIM), P(None, DIM), P(DIM, None), P()),
        out_specs=(P(BATCH), P(BATCH, DIM), P(DIM, BATCH)),
        check_vma=False,
    )
```

```python
import math

import jax
import jax.numpy as jnp
from jax import lax
from jax.experimental import pallas as pl
from jax.experimental.pallas import tpu as pltpu
from jax.sharding import Mesh
from jax.sharding import PartitionSpec as P

D = 4096
STEPS = 3
B = 256
H = B // 2
Q = B // 4
CHAINS = 2 * STEPS
DIM = ("y", "x")
BATCH = ("z", "c")
MESH = pl.DeviceIdType.MESH
f32, bf16 = jnp.float32, jnp.bfloat16

time_step = 1.0 / 64.0
lam_coef = 50.0
noise_coef = math.sqrt(2.0)
zscale = 2.0 / math.sqrt(D)
ARRIVALS = 170
LEAVING = 48


def place(pos, extent):
    return pl.ds(pl.multiple_of(pos * extent, extent), extent)


class Net:

    def __init__(self, send, recv):
        self.send, self.recv, self.count, self.begun, self.seen = send, recv, 0, [], set()

    def slots(self, count):
        self.count += count
        assert self.count <= ARRIVALS
        return [self.recv.at[k] for k in range(self.count - count, self.count)]

    def copy(self, src, dst, device, slot=None):
        return (src, dst, device, self.slots(1)[0] if slot is None else slot)

    def made(self, copy, send):
        src, dst, device, slot = copy
        return pltpu.make_async_remote_copy(
            src_ref=src, dst_ref=dst, send_sem=send, recv_sem=slot, device_id=device, device_id_type=MESH
        )

    def start(self, copy):
        send = self.send.at[len(self.begun) % LEAVING]
        if len(self.begun) >= LEAVING:
            self.begun[len(self.begun) - LEAVING].wait_send()
        made = self.made(copy, send)
        made.start()
        self.begun.append(made)

    def arrived(self, copy):
        if id(copy) not in self.seen:
            self.seen.add(id(copy))
            self.made(copy, self.send.at[0]).wait_recv()

    def drain(self):
        for copy in self.begun[-LEAVING:]:
            copy.wait_send()


class Gather:

    def __init__(self, net, axis, view, four, slots=None):
        p = lax.axis_index(axis)
        r, l = lax.rem(p + 1, 4), lax.rem(p + 3, 4)
        self.net, self.slots = net, slots or net.slots(3)
        self.copies = [
            net.copy(view(owner, half), view(owner, half), {axis: to}, self.slots[min(k, 2)])
            for k, (owner, half, to) in enumerate(((p, 0, r), (p, 1, l), (p, 1, r), (p, 0, l), (l, 0, r), (r, 1, l)))
        ]
        self.rest = (four, four, {axis: r}, self.slots[2])

    def start(self):
        for k in range(4):
            self.net.start(self.copies[k])

    def mid(self):
        for k in range(2):
            self.net.arrived(self.copies[k])
            self.net.start(self.copies[4 + k])

    def finish(self):
        self.net.arrived(self.rest)


class Scatter:

    def __init__(self, net, axis, sent, far, near, held, slots=None):
        p = lax.axis_index(axis)
        r, l = {axis: lax.rem(p + 1, 4)}, {axis: lax.rem(p + 3, 4)}
        self.net, self.sent, self.far, self.near, self.held = net, sent, far, near, held
        self.slots = slots or net.slots(3)
        a, b, rest = self.slots
        self.copies = {
            (2, 0): net.copy(sent.at[1, 0], far.at[0], r, a),
            (2, 1): net.copy(sent.at[1, 1], far.at[1], l, b),
            (1, 1): net.copy(sent.at[0, 1], near.at[0, 1], r, rest),
            (3, 0): net.copy(sent.at[2, 0], near.at[1, 0], l, rest),
            (1, 0): net.copy(sent.at[0, 0], near.at[0, 0], r, rest),
            (3, 1): net.copy(sent.at[2, 1], near.at[1, 1], l, rest),
        }
        self.rest = (near, near, r, rest)

    def put(self, k, half, value):
        if (k, half) in ((2, 0), (2, 1), (1, 1), (3, 0)):
            self.sent[k - 1, half] = value.astype(bf16)
            self.net.start(self.copies[k, half])
        else:
            self.held[{0: half, 1: 2, 3: 3}[k]] = value

    def mid(self):
        for side, key in enumerate(((1, 0), (3, 1))):
            self.net.arrived(self.copies[2, side])
            k, half = key
            self.sent[k - 1, half] = (self.held[2 + side] + self.far[side].astype(f32)).astype(bf16)
            self.net.start(self.copies[key])

    def finish(self):
        self.net.arrived(self.rest)
        near = self.near
        return [self.held[half] + near[0, half].astype(f32) + near[1, half].astype(f32) for half in range(2)]


ORDER = (2, 1, 3, 0)
PROGRAM = [
    "w1a2", "w1a1", "gx0.mid", "w1b2", "gx1.mid", "w1c2", "w1b0", "w1a0", "gx3.mid", "w1b1", "w1c1", "w2a1", "f01",
    "w2a0", "f02", "w1c0", "f32", "gx2.mid", "f30", "f11", "f12", "gx5.mid", "f00", "f03", "f31", "w2a2", "f33",
    "sh0.mid", "w2b1", "sh3.mid", "f13", "gx4.mid", "f22", "w2b0", "sh1.mid", "w2b2", "act0", "w2c1", "f20", "f10",
    "act3", "f21", "w2c0", "ga0.mid", "act1", "w2c2", "ga3.mid", "f23", "sh2.mid", "f50", "s02", "s01", "f52", "s03",
    "ga1.mid", "f51", "f42", "s32", "act2", "s33", "s00", "sz0.mid", "f53", "s31", "sh5.mid", "f41", "s12", "f43",
    "sz3.mid", "sh4.mid", "s11", "ga2.mid", "s13", "con0", "s10", "act5", "sz1.mid", "f40", "s30", "con3", "act4",
    "s22", "gu0.mid", "ga5.mid", "con1", "s21", "s23", "ga4.mid", "sz2.mid", "gu3.mid", "s52", "gu1.mid", "s42",
    "s20", "con2", "s53", "s51", "t32", "t03", "sz5.mid", "s41", "s43", "sz4.mid", "t12", "t31", "s50", "gu2.mid",
    "t11", "t02", "t13", "t33", "con5", "s40", "t01", "con4", "sg3.mid", "sg1.mid", "tot", "t22", "t23", "t20", "t21",
    "sg0.mid", "gu5.mid", "t10", "gu4.mid", "t00", "tot2", "sg2.mid", "t52", "t51", "t42", "t43", "t41", "t53", "res",
    "hid0", "t30", "hid1", "sg5.mid", "hid3", "sg4.mid", "resp", "sc0", "t50", "sc5", "sc2", "sc4", "sc1", "sc3",
    "hid2", "go0", "go1", "po02", "po12", "hid5", "t40", "hid4", "po03", "gg2.mid", "po01", "gg5.mid", "po10", "po11",
    "gg0.mid", "po00", "po13", "gg1.mid", "gg4.mid", "zo0.mid", "gg3.mid", "zo1.mid", "gs5", "gs2", "gs0", "gs1",
    "gs4", "gs3", "gi1", "gi0", "gj0", "gj1", "pi12", "pi02", "pi11", "pi13", "zi1.mid", "zo1.fin", "pi03", "pi01",
    "zi0.mid", "pi00", "zo0.fin", "pi10", "zi1.fin", "zi0.fin", "colo", "coli",
]


def dot(a, b, dims):
    return lax.dot_general(a, b, (dims, ((), ())), preferred_element_type=f32)


def kernel(
    start_in, inc_in, w_in, w_out, initial_in,
    res_out, grads_out,
    start, inc, xs, us, acts, scaled, ghs, w1, w2, slopes,
    sent, far, near, held, acc, zsent, zfar, zheld, znear,
    leave, totals, nrow, folded, resrow, rowres, give1, give2, initial, send, recv, local,
):
    y, x, z, c = (lax.axis_index(a) for a in ("y", "x", "z", "c"))

    barrier = pltpu.get_barrier_semaphore()
    peers = [{a: lax.rem(i + k, 4)} for a, i in (("x", x), ("y", y)) for k in (1, 2, 3)]
    peers += [{"z": lax.rem(z + k, 4)} for k in (1, 3)]
    peers += [{"c": 1 - c}] + [{"x": lax.rem(x + k, 4), "c": 1 - c} for k in (1, 2, 3)]
    for peer in peers:
        pl.semaphore_signal(barrier, inc=1, device_id=peer, device_id_type=MESH)

    fetch = [pltpu.make_async_copy(start_in, start, local.at[0])]
    fetch += [pltpu.make_async_copy(inc_in.at[n], inc.at[n], local.at[1 + n]) for n in range(STEPS)]
    own1 = [pltpu.make_async_copy(w_in.at[:, x], w1.at[x], local.at[4])]
    own2 = []
    for j in range(4):
        cols = pl.ds(pl.multiple_of(1024 * j + x * B, B), B)
        own2.append(pltpu.make_async_copy(w_out.at[:, :, cols], w2.at[j, x], local.at[5 + j]))
    gift1 = pltpu.make_async_copy(w_in.at[z, :, c], give1.at[0], local.at[9])
    over = lax.rem(z + 2, 4)
    gift3 = pltpu.make_async_copy(w_in.at[over, :, c], give1.at[1], local.at[21])
    gift2 = pltpu.make_async_copy(w_out.at[c, :, pl.ds(pl.multiple_of(z * 1024, 1024), 1024)], give2, local.at[10])
    scalar = pltpu.make_async_copy(initial_in, initial, local.at[11])
    for copy in [gift1, gift3] + fetch + [gift2] + own1 + own2 + [scalar]:
        copy.start()

    net = Net(send, recv)
    partner = {"c": 1 - c}

    def states_of(ref, n):
        return lambda owner, half: ref.at[n // 2, c, pl.ds(n % 2 * H + half * Q, Q), place(owner, B)]

    def hidden_of(ref, n):
        return lambda owner, half: ref.at[owner, n // 2, c, pl.ds(n % 2 * H + half * Q, Q)]

    def span(n):
        return pl.ds(n % 2 * H, H)

    def quarters(n):
        return [(half, pl.ds(n % 2 * H + half * Q, Q)) for half in range(2)]

    def piece(m, i, j):
        return w1.at[i, j, c] if m == 1 else w2.at[j, i, c]

    def quarter(m, i):
        return lambda owner, half: piece(m, i, owner).at[pl.ds(half * 64, 64)]

    four = acts.at[0, 0, 0]
    gx = [Gather(net, "y", states_of(xs, n), four) for n in range(CHAINS)]
    others = [lax.rem(x + k, 4) for k in (1, 2, 3)]
    froms = [lax.rem(x + 4 - k, 4) for k in (1, 2, 3)]
    ws, wz, wd = {}, {}, {}
    for m in (1, 2):
        for k, i in enumerate(others):
            src = give1.at[0, i] if m == 1 else give2.at[:, place(i, B)]
            ws[m, k] = net.copy(src, piece(m, x, z), {"x": i})
        for k, i in enumerate(froms):
            if m == 2:
                wz[m, k] = Gather(net, "z", quarter(m, i), four)
            slot = net.slots(1)[0]
            for t in range(4):
                mine = piece(m, i, lax.rem(z + t, 4))
                wd[m, k, t] = net.copy(mine, mine, {"c": 1 - c}, slot)
            whole = w1.at[i, :, c] if m == 1 else w2.at[:, i, c]
            wd[m, k] = (whole, whole, {"c": 1 - c}, slot)

    wr = [net.copy(give1.at[1, i], piece(1, x, over), {"x": i}) for i in others]
    up, down = lax.rem(z + 1, 4), lax.rem(z + 3, 4)
    wn = [[net.copy(piece(1, i, z), piece(1, i, z), {"z": to}) for to in (up, down)] for i in froms]

    def scatter(axis, k, slots=None):
        return Scatter(net, axis, sent.at[k], far.at[k], near.at[k], held.at[k], slots)

    sh = [scatter("x", n) for n in range(CHAINS)]
    sz = [scatter("y", CHAINS + n) for n in range(CHAINS)]
    sg = [scatter("x", 2 * CHAINS + n, sh[n].slots) for n in range(CHAINS)]
    ga = [Gather(net, "x", hidden_of(acts, n), four) for n in range(CHAINS)]
    gu = [Gather(net, "y", states_of(us, n), four, gx[n].slots) for n in range(CHAINS)]
    gg = [Gather(net, "x", hidden_of(ghs, n), four, ga[n].slots) for n in range(CHAINS)]
    over_y, over_x = net.slots(2)
    ty = [net.copy(totals.at[0, y], totals.at[0, y], {"y": lax.rem(y + k, 4)}, over_y) for k in (1, 2, 3)]
    tx = [net.copy(totals.at[1, x], totals.at[1, x], {"x": lax.rem(x + k, 4)}, over_x) for k in (1, 2, 3)]
    three = totals.at[0, pl.ds(0, 3)]
    ty_all, tx_all = (three, three, partner, over_y), (three, three, partner, over_x)
    def to_partner(ref):
        return net.copy(ref, ref, partner)

    def pair_to_partner(ref, n):
        slot = net.slots(1)[0]
        pair = [ref.at[2 * (1 - c) + e, n // 2, c, span(n)] for e in range(2)]
        both = ref.at[pl.ds(2 * c, 2), n // 2, 1 - c, span(n)]
        return [(p, p, partner, slot) for p in pair], (both, both, partner, slot)

    dx = [[to_partner(xs.at[n // 2, c, span(n)])] for n in range(CHAINS)]
    du = [[to_partner(us.at[n // 2, c, span(n)])] for n in range(CHAINS)]
    da = [pair_to_partner(acts, n) for n in range(CHAINS)]
    dg = [pair_to_partner(ghs, n) for n in range(CHAINS)]
    dr = to_partner(resrow.at[c])
    zs = [
        [Scatter(net, "z", zsent.at[g, r], zfar.at[g, r], znear.at[g, r], zheld.at[g, r]) for r in range(2)] for g in range(2)
    ]

    def per_path(t):
        return jnp.sum(t.T, axis=0, keepdims=True)

    with jax.named_scope("barrier"):
        pl.semaphore_wait(barrier, len(peers))
    gift1.wait()
    for k in (1, 0, 2):
        net.start(ws[1, k])
    gift3.wait()
    for k in (0, 2, 1):
        net.start(wr[k])
    fetch[0].wait()
    state = start[...]
    for n in range(STEPS):
        xs[n, c, :, place(y, B)] = state.astype(bf16)
        gx[2 * n].start()
        gx[2 * n + 1].start()
        if n == 0:
            gift2.wait()
            for k in (1, 0, 2):
                net.start(ws[2, k])
        fetch[1 + n].wait()
        state = state + noise_coef * inc[n]
    norm = state * state
    nrow[...] = per_path(norm[:, :128] + norm[:, 128:])
    scalar.wait()

    def put_both(scatter_sum, k, part):
        for half in range(2):
            scatter_sum.put(k, half, part[half * Q : half * Q + Q])

    ready = set()

    def share(key, copies):
        if key not in ready:
            ready.add(key)
            for copy in copies:
                net.start(copy)

    def wait_once(copies):
        for copy in copies:
            if id(copy) not in ready:
                ready.add(id(copy))
                copy.wait()

    def weights(m, k):
        net.arrived(wd[m, k])

    def first(n, k):
        gx[n].finish()
        if k:
            weights(1, 3 - k)
        else:
            wait_once(own1)
        w = w1[lax.rem(x + k, 4)].reshape(4 * B, B)
        put_both(sh[n], k, dot(xs[n // 2, c, span(n)], w, ((1,), (0,))))
        share(("x", n), dx[n])

    def second(n, k):
        ga[n].finish()
        for e in range(3):
            weights(2, e)
        wait_once(own2)
        j = lax.rem(y + k, 4)
        part = None
        for i in range(4):
            term = dot(acts[i, n // 2, c, span(n)], w2[j, i].reshape(B, B), ((1,), (0,)))
            part = term if part is None else part + term
        put_both(sz[n], k, part)
        share(("a", n), da[n][0])

    def third(n, k):
        gu[n].finish()
        i = lax.rem(x + k, 4)
        part = None
        for j in range(4):
            term = dot(us[n // 2, c, span(n), pl.ds(j * B, B)], w2[j, i].reshape(B, B), ((1,), (1,)))
            part = term if part is None else part + term
        put_both(sg[n], k, part)
        share(("u", n), du[n])

    def activate(n):
        for (half, at), h in zip(quarters(n), sh[n].finish()):
            sig = jax.nn.sigmoid(h)
            acts[x, n // 2, c, at] = (h * sig).astype(bf16)
            slopes[n, half] = sig * (1.0 + h * (1.0 - sig))
        ga[n].start()

    begun = set()

    def control(n):
        for (half, at), total in zip(quarters(n), sz[n].finish()):
            zval = zscale * total
            dw = inc[n // 2, at, :]
            us[n // 2, c, at, place(y, B)] = (zscale * (lam_coef * time_step * zval + dw)).astype(bf16)
            term = 0.5 * lam_coef * time_step * zval * zval + zval * dw
            term = term[:, :128] + term[:, 128:]
            folded[at, :] = folded[at, :] + term if n % 2 in begun else term
        begun.add(n % 2)
        gu[n].start()

    def hidden_grad(n):
        for (half, at), g in zip(quarters(n), sg[n].finish()):
            r = rowres[c, at, :]
            r = jnp.concatenate([r, r], axis=1)
            ghs[x, n // 2, c, at] = (r * g * slopes[n, half]).astype(bf16)
        gg[n].start()

    def totals_y():
        y_row = per_path(folded[...])
        totals[0, y] = jnp.concatenate([y_row, nrow[...], jnp.zeros((6, B), f32)], axis=0)
        for copy in ty:
            net.start(copy)

    def totals_x():
        net.arrived(ty_all)
        totals[1, x] = totals[0, 0] + totals[0, 1] + totals[0, 2] + totals[0, 3]
        for copy in tx:
            net.start(copy)

    kept_row = pltpu.make_async_copy(resrow.at[c], res_out, local.at[12])

    def residuals():
        net.arrived(tx_all)
        both = totals[1, 0] + totals[1, 1] + totals[1, 2] + totals[1, 3]
        residual = initial[0] + both[0:1] - jnp.log((1.0 + both[1:2]) * 0.5)
        resrow[c] = jnp.broadcast_to(residual, (8, B))
        net.start(dr)
        kept_row.start()
        rowres[c] = jnp.broadcast_to(residual, (128, B)).T

    def partner_residuals():
        net.arrived(dr)
        rowres[1 - c] = jnp.broadcast_to(resrow[1 - c, 0:1], (128, B)).T

    def scale(n):
        net.arrived(da[n][1])
        for e in range(2):
            for core in range(2):
                for k in range(2):
                    lanes = pl.ds(k * 128, 128)
                    a = acts[2 * c + e, n // 2, core, span(n), lanes].astype(f32)
                    scaled[e, n // 2, core, span(n), lanes] = (a * rowres[core, span(n)]).astype(bf16)

    def out_sum(e):
        for n in range(CHAINS):
            gu[n].finish()
            for copy in du[n]:
                net.arrived(copy)
        every = STEPS * 2 * B
        acc[1, e] = dot(scaled[e].reshape(every, B), us[...].reshape(every, 4 * B), ((0,), (0,)))

    def give(n):
        gg[n].finish()
        for copy in dg[n][0]:
            net.start(copy)

    def of_chain(e, n):
        for copy in dx[n] + [dg[n][1]]:
            net.arrived(copy)
        g = ghs[2 * c + e, n // 2, :, span(n)].reshape(B, B)
        return dot(g, xs[n // 2, :, span(n)].reshape(B, 4 * B), ((0,), (0,)))

    def in_sum(e):
        for n in range(4):
            for copy in dx[n] + [dg[n][1]]:
                net.arrived(copy)
        g = ghs[2 * c + e, pl.ds(0, 2)].reshape(4 * B, B)
        acc[0, e] = dot(g, xs[pl.ds(0, 2)].reshape(4 * B, 4 * B), ((0,), (0,))) + of_chain(e, 4)

    def in_last(e):
        acc[0, e] = acc[0, e] + of_chain(e, 5)

    def over_z(g, r, k):
        cols = place(lax.rem(z + k, 4), B)
        for e in range(2):
            zs[g][r].put(k, e, acc[g, e, pl.ds(r * H, H), cols])

    def leaving(g, r, e, slot):
        rows = pl.ds(r * H, H)
        k = 4 * g + 2 * r
        return pltpu.make_async_remote_copy(
            src_ref=leave.at[g, e, rows],
            dst_ref=grads_out.at[g, slot, rows],
            send_sem=send.at[LEAVING + k + e],
            recv_sem=recv.at[ARRIVALS + k + slot],
            device_id={"x": 2 * c + e, "c": x // 2},
            device_id_type=MESH,
        )

    def staying(g, r, e):
        rows = pl.ds(r * H, H)
        return pltpu.make_async_copy(leave.at[g, e, rows], grads_out.at[g, e, rows], local.at[13 + 4 * g + 2 * r + e])

    def to_owner(g, r):
        for e, value in enumerate(zs[g][r].finish()):
            leave[g, e, pl.ds(r * H, H)] = value.astype(bf16)

            @pl.when(2 * c + e != x)
            def _(e=e):
                leaving(g, r, e, lax.rem(x, 2)).start()

            @pl.when(2 * c + e == x)
            def _(e=e):
                staying(g, r, e).start()

    def collect(g):
        for r in range(2):
            for e in range(2):

                @pl.when(2 * c + e != x)
                def _(r=r, e=e):
                    copy = leaving(g, r, e, e)
                    copy.wait_recv()
                    copy.wait_send()

                @pl.when(2 * c + e == x)
                def _(r=r, e=e):
                    staying(g, r, e).wait()

    def weights_in(m, k):
        net.arrived(ws[m, k])
        if m == 1:
            for copy in wn[k]:
                net.start(copy)
        else:
            wz[m, k].start()
        net.start(wd[m, k, 0])

    def straight_in(k):
        net.arrived(wr[k])
        net.start(wd[1, k, 2])

    def weights_out(m, k):
        if m == 1:
            for t, copy in ((3, wn[k][0]), (1, wn[k][1])):
                net.arrived(copy)
                net.start(wd[m, k, t])
        else:
            wz[m, k].finish()
            for t in (1, 3, 2):
                net.start(wd[m, k, t])

    tasks = {"tot": totals_y, "tot2": totals_x, "res": residuals, "resp": partner_residuals}
    for m in (1, 2):
        for k in range(3):
            tasks[f"w{m}a{k}"] = lambda m=m, k=k: weights_in(m, k)
            tasks[f"w{m}b{k}"] = (lambda k=k: straight_in(k)) if m == 1 else wz[m, k].mid
            tasks[f"w{m}c{k}"] = lambda m=m, k=k: weights_out(m, k)
    for n in range(CHAINS):
        for k in range(4):
            tasks[f"f{n}{k}"] = lambda n=n, k=k: first(n, k)
            tasks[f"s{n}{k}"] = lambda n=n, k=k: second(n, k)
            tasks[f"t{n}{k}"] = lambda n=n, k=k: third(n, k)
        named = {"gx": gx, "sh": sh, "ga": ga, "sz": sz, "gu": gu, "sg": sg, "gg": gg}
        for name, ops in named.items():
            tasks[f"{name}{n}.mid"] = ops[n].mid
        tasks[f"act{n}"] = lambda n=n: activate(n)
        tasks[f"con{n}"] = lambda n=n: control(n)
        tasks[f"hid{n}"] = lambda n=n: hidden_grad(n)
        tasks[f"sc{n}"] = lambda n=n: scale(n)
        tasks[f"gs{n}"] = lambda n=n: give(n)

    for e in range(2):
        tasks[f"go{e}"] = lambda e=e: out_sum(e)
        tasks[f"gi{e}"] = lambda e=e: in_sum(e)
        tasks[f"gj{e}"] = lambda e=e: in_last(e)
    for g, name in enumerate("io"):
        for r in range(2):
            for k in range(4):
                tasks[f"p{name}{r}{k}"] = lambda g=g, r=r, k=k: over_z(g, r, k)
            tasks[f"z{name}{r}.mid"] = zs[g][r].mid
            tasks[f"z{name}{r}.fin"] = lambda g=g, r=r: to_owner(g, r)
        tasks[f"col{name}"] = lambda g=g: collect(g)

    assert sorted(PROGRAM) == sorted(tasks)
    for name in PROGRAM:
        with jax.named_scope(name):
            tasks[name]()
    kept_row.wait()
    net.drain()


def placing(row, blocks, residual, grad_in, grad_out):
    residual[...] = row[0:1].reshape(B)
    for t in range(2):
        grad_in[pl.ds(t * B, B), :] = blocks[0, t].astype(f32).T
        grad_out[:, pl.ds(t * B, B)] = blocks[1, t].astype(f32)


def on_device(start, increments, w_in, w_out, initial):
    vmem, anywhere = pl.BlockSpec(memory_space=pltpu.VMEM), pl.BlockSpec(memory_space=pl.ANY)
    states = pltpu.VMEM((STEPS, 2, B, 4 * B), bf16)
    hidden = pltpu.VMEM((4, STEPS, 2, B, B), bf16)
    weights = pltpu.VMEM((4, 4, 2, H, B), bf16)
    row, blocks = pl.pallas_call(
        kernel,
        out_shape=(jax.ShapeDtypeStruct((8, B), f32), jax.ShapeDtypeStruct((2, 2, B, B), bf16)),
        in_specs=[anywhere] * 5,
        out_specs=(anywhere, anywhere),
        scratch_shapes=[
            pltpu.VMEM((B, B), f32),
            pltpu.VMEM((STEPS, B, B), f32),
            states,
            states,
            hidden,
            pltpu.VMEM((2, STEPS, 2, B, B), bf16),
            hidden,
            weights,
            weights,
            pltpu.VMEM((CHAINS, 2, Q, B), f32),
            pltpu.VMEM((3 * CHAINS, 3, 2, Q, B), bf16),
            pltpu.VMEM((3 * CHAINS, 2, Q, B), bf16),
            pltpu.VMEM((3 * CHAINS, 2, 2, Q, B), bf16),
            pltpu.VMEM((3 * CHAINS, 4, Q, B), f32),
            pltpu.VMEM((2, 2, B, 4 * B), f32),
            pltpu.VMEM((2, 2, 3, 2, H, B), bf16),
            pltpu.VMEM((2, 2, 2, H, B), bf16),
            pltpu.VMEM((2, 2, 4, H, B), f32),
            pltpu.VMEM((2, 2, 2, 2, H, B), bf16),
            pltpu.VMEM((2, 2, B, B), bf16),
            pltpu.VMEM((2, 4, 8, B), f32),
            pltpu.VMEM((1, B), f32),
            pltpu.VMEM((B, 128), f32),
            pltpu.VMEM((2, 8, B), f32),
            pltpu.VMEM((2, B, 128), f32),
            pltpu.VMEM((2, 4, H, B), bf16),
            pltpu.VMEM((H, 4 * B), bf16),
            pltpu.SMEM((1,), f32),
            pltpu.SemaphoreType.DMA((LEAVING + 8,)),
            pltpu.SemaphoreType.DMA((ARRIVALS + 8,)),
            pltpu.SemaphoreType.DMA((22,)),
        ],
        compiler_params=pltpu.CompilerParams(collective_id=0, has_side_effects=True, vmem_limit_bytes=66000000),
    )(start, increments, w_in.reshape(4, 4, 2, H, B), w_out.reshape(2, H, D), initial.reshape(1))
    return pl.pallas_call(
        placing,
        out_shape=(
            jax.ShapeDtypeStruct((B,), f32),
            jax.ShapeDtypeStruct((2 * B, B), f32),
            jax.ShapeDtypeStruct((B, 2 * B), f32),
        ),
        in_specs=[vmem, vmem],
        out_specs=(vmem, vmem, vmem),
    )(row, blocks)


def solution(mesh):
    finer = Mesh(mesh.devices.reshape(4, 4, 4, 2), ("y", "x", "z", "c"))
    return jax.shard_map(
        on_device,
        mesh=finer,
        in_specs=(P(BATCH, DIM), P(None, BATCH, DIM), P(None, DIM), P(DIM, None), P()),
        out_specs=(P(BATCH), P(BATCH, DIM), P(DIM, BATCH)),
        check_vma=False,
    )
```

```python
import math

import jax
import jax.numpy as jnp
from jax import lax
from jax.experimental import pallas as pl
from jax.experimental.pallas import tpu as pltpu
from jax.sharding import Mesh
from jax.sharding import PartitionSpec as P

D = 4096
STEPS = 3
B = 256
H = B // 2
Q = B // 4
CHAINS = 2 * STEPS
DIM = ("y", "x")
BATCH = ("z", "c")
MESH = pl.DeviceIdType.MESH
f32, bf16 = jnp.float32, jnp.bfloat16

time_step = 1.0 / 64.0
lam_coef = 50.0
noise_coef = math.sqrt(2.0)
zscale = 2.0 / math.sqrt(D)
ARRIVALS = 141
LEAVING = 40


def place(pos, extent):
    return pl.ds(pl.multiple_of(pos * extent, extent), extent)


class Net:

    def __init__(self, send, recv):
        self.send, self.recv, self.count, self.begun, self.seen = send, recv, 0, [], set()

    def slots(self, count):
        self.count += count
        assert self.count <= ARRIVALS
        return [self.recv.at[k] for k in range(self.count - count, self.count)]

    def copy(self, src, dst, device, slot=None):
        return (src, dst, device, self.slots(1)[0] if slot is None else slot)

    def made(self, copy, send):
        src, dst, device, slot = copy
        return pltpu.make_async_remote_copy(
            src_ref=src, dst_ref=dst, send_sem=send, recv_sem=slot, device_id=device, device_id_type=MESH
        )

    def start(self, copy):
        send = self.send.at[len(self.begun) % LEAVING]
        if len(self.begun) >= LEAVING:
            self.begun[len(self.begun) - LEAVING].wait_send()
        made = self.made(copy, send)
        made.start()
        self.begun.append(made)

    def arrived(self, copy):
        if id(copy) not in self.seen:
            self.seen.add(id(copy))
            self.made(copy, self.send.at[0]).wait_recv()

    def drain(self):
        for copy in self.begun[-LEAVING:]:
            copy.wait_send()


class Gather:

    def __init__(self, net, axis, view, four, slots=None):
        p = lax.axis_index(axis)
        r, l = lax.rem(p + 1, 4), lax.rem(p + 3, 4)
        self.net, self.slots = net, slots or net.slots(3)
        self.copies = [
            net.copy(view(owner, half), view(owner, half), {axis: to}, self.slots[min(k, 2)])
            for k, (owner, half, to) in enumerate(((p, 0, r), (p, 1, l), (p, 1, r), (p, 0, l), (l, 0, r), (r, 1, l)))
        ]
        self.rest = (four, four, {axis: r}, self.slots[2])

    def start(self):
        for k in range(4):
            self.net.start(self.copies[k])

    def mid(self):
        for k in range(2):
            self.net.arrived(self.copies[k])
            self.net.start(self.copies[4 + k])

    def finish(self):
        self.net.arrived(self.rest)


class Scatter:

    def __init__(self, net, axis, sent, far, near, held, slots=None):
        p = lax.axis_index(axis)
        r, l = {axis: lax.rem(p + 1, 4)}, {axis: lax.rem(p + 3, 4)}
        self.net, self.sent, self.far, self.near, self.held = net, sent, far, near, held
        self.slots = slots or net.slots(3)
        a, b, rest = self.slots
        self.copies = {
            (2, 0): net.copy(sent.at[1, 0], far.at[0], r, a),
            (2, 1): net.copy(sent.at[1, 1], far.at[1], l, b),
            (1, 1): net.copy(sent.at[0, 1], near.at[0, 1], r, rest),
            (3, 0): net.copy(sent.at[2, 0], near.at[1, 0], l, rest),
            (1, 0): net.copy(sent.at[0, 0], near.at[0, 0], r, rest),
            (3, 1): net.copy(sent.at[2, 1], near.at[1, 1], l, rest),
        }
        self.rest = (near, near, r, rest)

    def put(self, k, half, value):
        if (k, half) in ((2, 0), (2, 1), (1, 1), (3, 0)):
            self.sent[k - 1, half] = value.astype(bf16)
            self.net.start(self.copies[k, half])
        else:
            self.held[{0: half, 1: 2, 3: 3}[k]] = value

    def mid(self):
        for side, key in enumerate(((1, 0), (3, 1))):
            self.net.arrived(self.copies[2, side])
            k, half = key
            self.sent[k - 1, half] = (self.held[2 + side] + self.far[side].astype(f32)).astype(bf16)
            self.net.start(self.copies[key])

    def finish(self):
        self.net.arrived(self.rest)
        near = self.near
        return [self.held[half] + near[0, half].astype(f32) + near[1, half].astype(f32) for half in range(2)]


ORDER = (2, 1, 3, 0)
PROGRAM = [
    "w1a2", "w1a1", "gx0.mid", "w1b2", "gx1.mid", "w1c2", "w1b0", "w1a0", "gx3.mid", "w1b1", "w1c1", "w2a1", "f01",
    "w2a0", "f02", "w1c0", "f32", "gx2.mid", "f30", "f11", "f12", "gx5.mid", "f00", "f03", "f31", "w2a2", "f33",
    "sh0.mid", "w2b1", "sh3.mid", "f13", "gx4.mid", "f22", "w2b0", "sh1.mid", "w2b2", "act0", "w2c1", "f20", "f10",
    "act3", "f21", "w2c0", "ga0.mid", "act1", "w2c2", "ga3.mid", "f23", "sh2.mid", "f50", "s02", "s01", "f52", "s03",
    "ga1.mid", "f51", "f42", "s32", "act2", "s33", "s00", "sz0.mid", "f53", "s31", "sh5.mid", "f41", "s12", "f43",
    "sz3.mid", "sh4.mid", "s11", "ga2.mid", "s13", "con0", "s10", "act5", "sz1.mid", "f40", "s30", "con3", "act4",
    "s22", "gu0.mid", "ga5.mid", "con1", "s21", "s23", "ga4.mid", "sz2.mid", "gu3.mid", "s52", "gu1.mid", "s42",
    "s20", "con2", "s53", "s51", "t32", "t03", "sz5.mid", "s41", "s43", "sz4.mid", "t12", "t31", "s50", "gu2.mid",
    "t11", "t02", "t13", "t33", "con5", "s40", "t01", "con4", "sg3.mid", "sg1.mid", "tot", "t22", "t23", "t20", "t21",
    "sg0.mid", "gu5.mid", "t10", "gu4.mid", "t00", "tot2", "sg2.mid", "t52", "t51", "t42", "t43", "t41", "t53", "res",
    "hid0", "t30", "hid1", "sg5.mid", "hid3", "sg4.mid", "resp", "sc0", "t50", "sc5", "sc2", "sc4", "sc1", "sc3",
    "hid2", "go0", "go1", "po02", "po12", "hid5", "t40", "hid4", "po03", "gg2.mid", "po01", "gg5.mid", "po10", "po11",
    "gg0.mid", "po00", "po13", "gg1.mid", "gg4.mid", "zo0.mid", "gg3.mid", "zo1.mid", "gs5", "gs2", "gs0", "gs1",
    "gs4", "gs3", "gi1", "gi0", "gj0", "gj1", "pi12", "pi02", "pi11", "pi13", "pi03", "pi01", "pi10", "pi00",
    "zi1.mid", "zo1.fin", "zi0.mid", "zo0.fin", "zi1.fin", "zi0.fin", "colo", "coli",
]


def dot(a, b, dims):
    return lax.dot_general(a, b, (dims, ((), ())), preferred_element_type=f32)


def kernel(
    start_in, inc_in, w_in, w_out, initial_in,
    res_out, grads_out,
    start, inc, xs, us, acts, scaled, ghs, w1, w2, slopes,
    sent, far, near, held, acc, zsent, zfar, zheld, znear,
    leave, totals, nrow, folded, resrow, rowres, give1, give2, initial, send, recv, local,
):
    y, x, z, c = (lax.axis_index(a) for a in ("y", "x", "z", "c"))

    barrier = pltpu.get_barrier_semaphore()
    peers = [{a: lax.rem(i + k, 4)} for a, i in (("x", x), ("y", y)) for k in (1, 2, 3)]
    peers += [{"z": lax.rem(z + k, 4)} for k in (1, 3)]
    peers += [{"c": 1 - c}] + [{"x": lax.rem(x + k, 4), "c": 1 - c} for k in (1, 2, 3)]
    for peer in peers:
        pl.semaphore_signal(barrier, inc=1, device_id=peer, device_id_type=MESH)

    fetch = [pltpu.make_async_copy(start_in, start, local.at[0])]
    fetch += [pltpu.make_async_copy(inc_in.at[n], inc.at[n], local.at[1 + n]) for n in range(STEPS)]
    own1 = [pltpu.make_async_copy(w_in.at[:, x], w1.at[x], local.at[4])]
    own2 = []
    for j in range(4):
        cols = pl.ds(pl.multiple_of(1024 * j + x * B, B), B)
        own2.append(pltpu.make_async_copy(w_out.at[:, :, cols], w2.at[j, x], local.at[5 + j]))
    gift1 = pltpu.make_async_copy(w_in.at[z, :, c], give1.at[0], local.at[9])
    over = lax.rem(z + 2, 4)
    gift3 = pltpu.make_async_copy(w_in.at[over, :, c], give1.at[1], local.at[21])
    gift2 = pltpu.make_async_copy(w_out.at[c, :, pl.ds(pl.multiple_of(z * 1024, 1024), 1024)], give2, local.at[10])
    scalar = pltpu.make_async_copy(initial_in, initial, local.at[11])
    for copy in [gift1, gift3] + fetch + [gift2] + own1 + own2 + [scalar]:
        copy.start()

    net = Net(send, recv)
    partner = {"c": 1 - c}

    def states_of(ref, n):
        return lambda owner, half: ref.at[n // 2, c, pl.ds(n % 2 * H + half * Q, Q), place(owner, B)]

    def hidden_of(ref, n):
        return lambda owner, half: ref.at[owner, n // 2, c, pl.ds(n % 2 * H + half * Q, Q)]

    def span(n):
        return pl.ds(n % 2 * H, H)

    def quarters(n):
        return [(half, pl.ds(n % 2 * H + half * Q, Q)) for half in range(2)]

    def piece(m, i, j):
        return w1.at[i, j, c] if m == 1 else w2.at[j, i, c]

    def quarter(m, i):
        return lambda owner, half: piece(m, i, owner).at[pl.ds(half * 64, 64)]

    four = acts.at[0, 0, 0]
    gx = [Gather(net, "y", states_of(xs, n), four) for n in range(CHAINS)]
    others = [lax.rem(x + k, 4) for k in (1, 2, 3)]
    froms = [lax.rem(x + 4 - k, 4) for k in (1, 2, 3)]
    ws, wz, wd = {}, {}, {}
    for m in (1, 2):
        for k, i in enumerate(others):
            src = give1.at[0, i] if m == 1 else give2.at[:, place(i, B)]
            ws[m, k] = net.copy(src, piece(m, x, z), {"x": i})
        for k, i in enumerate(froms):
            if m == 2:
                wz[m, k] = Gather(net, "z", quarter(m, i), four)
            slot = net.slots(1)[0]
            for t in range(4):
                mine = piece(m, i, lax.rem(z + t, 4))
                wd[m, k, t] = net.copy(mine, mine, {"c": 1 - c}, slot)
            whole = w1.at[i, :, c] if m == 1 else w2.at[:, i, c]
            wd[m, k] = (whole, whole, {"c": 1 - c}, slot)

    wr = [net.copy(give1.at[1, i], piece(1, x, over), {"x": i}) for i in others]
    up, down = lax.rem(z + 1, 4), lax.rem(z + 3, 4)
    wn = [[net.copy(piece(1, i, z), piece(1, i, z), {"z": to}) for to in (up, down)] for i in froms]

    def scatter(axis, k, slots=None):
        return Scatter(net, axis, sent.at[k], far.at[k], near.at[k], held.at[k], slots)

    sh = [scatter("x", n) for n in range(CHAINS)]
    sz = [scatter("y", CHAINS + n) for n in range(CHAINS)]
    sg = [scatter("x", 2 * CHAINS + n, sh[n].slots) for n in range(CHAINS)]
    ga = [Gather(net, "x", hidden_of(acts, n), four) for n in range(CHAINS)]
    gu = [Gather(net, "y", states_of(us, n), four, gx[n].slots) for n in range(CHAINS)]
    gg = [Gather(net, "x", hidden_of(ghs, n), four, ga[n].slots) for n in range(CHAINS)]
    over_y, over_x = net.slots(2)
    ty = [net.copy(totals.at[0, y], totals.at[0, y], {"y": lax.rem(y + k, 4)}, over_y) for k in (1, 2, 3)]
    tx = [net.copy(totals.at[1, x], totals.at[1, x], {"x": lax.rem(x + k, 4)}, over_x) for k in (1, 2, 3)]
    three = totals.at[0, pl.ds(0, 3)]
    ty_all, tx_all = (three, three, partner, over_y), (three, three, partner, over_x)
    def to_partner(ref):
        return net.copy(ref, ref, partner)

    def pair_to_partner(ref, n):
        slot = net.slots(1)[0]
        pair = [ref.at[2 * (1 - c) + e, n // 2, c, span(n)] for e in range(2)]
        both = ref.at[pl.ds(2 * c, 2), n // 2, 1 - c, span(n)]
        return [(p, p, partner, slot) for p in pair], (both, both, partner, slot)

    dx = [[to_partner(xs.at[n // 2, c, span(n)])] for n in range(CHAINS)]
    du = [[to_partner(us.at[n // 2, c, span(n)])] for n in range(CHAINS)]
    da = [pair_to_partner(acts, n) for n in range(CHAINS)]
    dg = [pair_to_partner(ghs, n) for n in range(CHAINS)]
    dr = to_partner(resrow.at[c])
    zs = [
        [Scatter(net, "z", zsent.at[g, r], zfar.at[g, r], znear.at[g, r], zheld.at[g, r]) for r in range(2)] for g in range(2)
    ]

    def per_path(t):
        return jnp.sum(t.T, axis=0, keepdims=True)

    with jax.named_scope("barrier"):
        pl.semaphore_wait(barrier, len(peers))
    gift1.wait()
    for k in (1, 0, 2):
        net.start(ws[1, k])
    gift3.wait()
    for k in (0, 2, 1):
        net.start(wr[k])
    fetch[0].wait()
    state = start[...]
    for n in range(STEPS):
        xs[n, c, :, place(y, B)] = state.astype(bf16)
        gx[2 * n].start()
        gx[2 * n + 1].start()
        if n == 0:
            gift2.wait()
            for k in (1, 0, 2):
                net.start(ws[2, k])
        fetch[1 + n].wait()
        state = state + noise_coef * inc[n]
    norm = state * state
    nrow[...] = per_path(norm[:, :128] + norm[:, 128:])
    scalar.wait()

    def put_both(scatter_sum, k, part):
        for half in range(2):
            scatter_sum.put(k, half, part[half * Q : half * Q + Q])

    ready = set()

    def share(key, copies):
        if key not in ready:
            ready.add(key)
            for copy in copies:
                net.start(copy)

    def wait_once(copies):
        for copy in copies:
            if id(copy) not in ready:
                ready.add(id(copy))
                copy.wait()

    def weights(m, k):
        net.arrived(wd[m, k])

    def first(n, k):
        gx[n].finish()
        if k:
            weights(1, 3 - k)
        else:
            wait_once(own1)
        w = w1[lax.rem(x + k, 4)].reshape(4 * B, B)
        put_both(sh[n], k, dot(xs[n // 2, c, span(n)], w, ((1,), (0,))))
        share(("x", n), dx[n])

    def second(n, k):
        ga[n].finish()
        for e in range(3):
            weights(2, e)
        wait_once(own2)
        j = lax.rem(y + k, 4)
        part = None
        for i in range(4):
            term = dot(acts[i, n // 2, c, span(n)], w2[j, i].reshape(B, B), ((1,), (0,)))
            part = term if part is None else part + term
        put_both(sz[n], k, part)
        share(("a", n), da[n][0])

    def third(n, k):
        gu[n].finish()
        i = lax.rem(x + k, 4)
        part = None
        for j in range(4):
            term = dot(us[n // 2, c, span(n), pl.ds(j * B, B)], w2[j, i].reshape(B, B), ((1,), (1,)))
            part = term if part is None else part + term
        put_both(sg[n], k, part)
        share(("u", n), du[n])

    def activate(n):
        for (half, at), h in zip(quarters(n), sh[n].finish()):
            sig = jax.nn.sigmoid(h)
            acts[x, n // 2, c, at] = (h * sig).astype(bf16)
            slopes[n, half] = sig * (1.0 + h * (1.0 - sig))
        ga[n].start()

    begun = set()

    def control(n):
        for (half, at), total in zip(quarters(n), sz[n].finish()):
            zval = zscale * total
            dw = inc[n // 2, at, :]
            us[n // 2, c, at, place(y, B)] = (zscale * (lam_coef * time_step * zval + dw)).astype(bf16)
            term = 0.5 * lam_coef * time_step * zval * zval + zval * dw
            term = term[:, :128] + term[:, 128:]
            folded[at, :] = folded[at, :] + term if n % 2 in begun else term
        begun.add(n % 2)
        gu[n].start()

    def hidden_grad(n):
        for (half, at), g in zip(quarters(n), sg[n].finish()):
            r = rowres[c, at, :]
            r = jnp.concatenate([r, r], axis=1)
            ghs[x, n // 2, c, at] = (r * g * slopes[n, half]).astype(bf16)
        gg[n].start()

    def totals_y():
        y_row = per_path(folded[...])
        totals[0, y] = jnp.concatenate([y_row, nrow[...], jnp.zeros((6, B), f32)], axis=0)
        for copy in ty:
            net.start(copy)

    def totals_x():
        net.arrived(ty_all)
        totals[1, x] = totals[0, 0] + totals[0, 1] + totals[0, 2] + totals[0, 3]
        for copy in tx:
            net.start(copy)

    kept_row = pltpu.make_async_copy(resrow.at[c], res_out, local.at[12])

    def residuals():
        net.arrived(tx_all)
        both = totals[1, 0] + totals[1, 1] + totals[1, 2] + totals[1, 3]
        residual = initial[0] + both[0:1] - jnp.log((1.0 + both[1:2]) * 0.5)
        resrow[c] = jnp.broadcast_to(residual, (8, B))
        net.start(dr)
        kept_row.start()
        rowres[c] = jnp.broadcast_to(residual, (128, B)).T

    def partner_residuals():
        net.arrived(dr)
        rowres[1 - c] = jnp.broadcast_to(resrow[1 - c, 0:1], (128, B)).T

    def scale(n):
        net.arrived(da[n][1])
        for e in range(2):
            for core in range(2):
                for k in range(2):
                    lanes = pl.ds(k * 128, 128)
                    a = acts[2 * c + e, n // 2, core, span(n), lanes].astype(f32)
                    scaled[e, n // 2, core, span(n), lanes] = (a * rowres[core, span(n)]).astype(bf16)

    def out_sum(e):
        for n in range(CHAINS):
            gu[n].finish()
            for copy in du[n]:
                net.arrived(copy)
        every = STEPS * 2 * B
        acc[1, e] = dot(scaled[e].reshape(every, B), us[...].reshape(every, 4 * B), ((0,), (0,)))

    def give(n):
        gg[n].finish()
        for copy in dg[n][0]:
            net.start(copy)

    def of_chain(e, n):
        for copy in dx[n] + [dg[n][1]]:
            net.arrived(copy)
        g = ghs[2 * c + e, n // 2, :, span(n)].reshape(B, B)
        return dot(g, xs[n // 2, :, span(n)].reshape(B, 4 * B), ((0,), (0,)))

    def in_sum(e):
        for n in range(4):
            for copy in dx[n] + [dg[n][1]]:
                net.arrived(copy)
        g = ghs[2 * c + e, pl.ds(0, 2)].reshape(4 * B, B)
        acc[0, e] = dot(g, xs[pl.ds(0, 2)].reshape(4 * B, 4 * B), ((0,), (0,))) + of_chain(e, 4)

    def in_last(e):
        acc[0, e] = acc[0, e] + of_chain(e, 5)

    def over_z(g, r, k):
        cols = place(lax.rem(z + k, 4), B)
        for e in range(2):
            zs[g][r].put(k, e, acc[g, e, pl.ds(r * H, H), cols])

    def leaving(g, r, e, slot):
        rows = pl.ds(r * H, H)
        k = 4 * g + 2 * r
        return pltpu.make_async_remote_copy(
            src_ref=leave.at[g, e, rows],
            dst_ref=grads_out.at[g, slot, rows],
            send_sem=send.at[LEAVING + k + e],
            recv_sem=recv.at[ARRIVALS + k + slot],
            device_id={"x": 2 * c + e, "c": x // 2},
            device_id_type=MESH,
        )

    def staying(g, r, e):
        rows = pl.ds(r * H, H)
        return pltpu.make_async_copy(leave.at[g, e, rows], grads_out.at[g, e, rows], local.at[13 + 4 * g + 2 * r + e])

    def to_owner(g, r):
        for e, value in enumerate(zs[g][r].finish()):
            leave[g, e, pl.ds(r * H, H)] = value.astype(bf16)

            @pl.when(2 * c + e != x)
            def _(e=e):
                leaving(g, r, e, lax.rem(x, 2)).start()

            @pl.when(2 * c + e == x)
            def _(e=e):
                staying(g, r, e).start()

    def collect(g):
        for r in range(2):
            for e in range(2):

                @pl.when(2 * c + e != x)
                def _(r=r, e=e):
                    copy = leaving(g, r, e, e)
                    copy.wait_recv()
                    copy.wait_send()

                @pl.when(2 * c + e == x)
                def _(r=r, e=e):
                    staying(g, r, e).wait()

    def weights_in(m, k):
        net.arrived(ws[m, k])
        if m == 1:
            for copy in wn[k]:
                net.start(copy)
        else:
            wz[m, k].start()
        net.start(wd[m, k, 0])

    def straight_in(k):
        net.arrived(wr[k])
        net.start(wd[1, k, 2])

    def weights_out(m, k):
        if m == 1:
            for t, copy in ((3, wn[k][0]), (1, wn[k][1])):
                net.arrived(copy)
                net.start(wd[m, k, t])
        else:
            wz[m, k].finish()
            for t in (1, 3, 2):
                net.start(wd[m, k, t])

    tasks = {"tot": totals_y, "tot2": totals_x, "res": residuals, "resp": partner_residuals}
    for m in (1, 2):
        for k in range(3):
            tasks[f"w{m}a{k}"] = lambda m=m, k=k: weights_in(m, k)
            tasks[f"w{m}b{k}"] = (lambda k=k: straight_in(k)) if m == 1 else wz[m, k].mid
            tasks[f"w{m}c{k}"] = lambda m=m, k=k: weights_out(m, k)
    for n in range(CHAINS):
        for k in range(4):
            tasks[f"f{n}{k}"] = lambda n=n, k=k: first(n, k)
            tasks[f"s{n}{k}"] = lambda n=n, k=k: second(n, k)
            tasks[f"t{n}{k}"] = lambda n=n, k=k: third(n, k)
        named = {"gx": gx, "sh": sh, "ga": ga, "sz": sz, "gu": gu, "sg": sg, "gg": gg}
        for name, ops in named.items():
            tasks[f"{name}{n}.mid"] = ops[n].mid
        tasks[f"act{n}"] = lambda n=n: activate(n)
        tasks[f"con{n}"] = lambda n=n: control(n)
        tasks[f"hid{n}"] = lambda n=n: hidden_grad(n)
        tasks[f"sc{n}"] = lambda n=n: scale(n)
        tasks[f"gs{n}"] = lambda n=n: give(n)

    for e in range(2):
        tasks[f"go{e}"] = lambda e=e: out_sum(e)
        tasks[f"gi{e}"] = lambda e=e: in_sum(e)
        tasks[f"gj{e}"] = lambda e=e: in_last(e)
    for g, name in enumerate("io"):
        for r in range(2):
            for k in range(4):
                tasks[f"p{name}{r}{k}"] = lambda g=g, r=r, k=k: over_z(g, r, k)
            tasks[f"z{name}{r}.mid"] = zs[g][r].mid
            tasks[f"z{name}{r}.fin"] = lambda g=g, r=r: to_owner(g, r)
        tasks[f"col{name}"] = lambda g=g: collect(g)

    assert sorted(PROGRAM) == sorted(tasks)
    for name in PROGRAM:
        with jax.named_scope(name):
            tasks[name]()
    kept_row.wait()
    net.drain()


def placing(row, blocks, residual, grad_in, grad_out):
    residual[...] = row[0:1].reshape(B)
    for t in range(2):
        grad_in[pl.ds(t * B, B), :] = blocks[0, t].astype(f32).T
        grad_out[:, pl.ds(t * B, B)] = blocks[1, t].astype(f32)


def on_device(start, increments, w_in, w_out, initial):
    vmem, anywhere = pl.BlockSpec(memory_space=pltpu.VMEM), pl.BlockSpec(memory_space=pl.ANY)
    states = pltpu.VMEM((STEPS, 2, B, 4 * B), bf16)
    hidden = pltpu.VMEM((4, STEPS, 2, B, B), bf16)
    weights = pltpu.VMEM((4, 4, 2, H, B), bf16)
    row, blocks = pl.pallas_call(
        kernel,
        out_shape=(jax.ShapeDtypeStruct((8, B), f32), jax.ShapeDtypeStruct((2, 2, B, B), bf16)),
        in_specs=[anywhere] * 5,
        out_specs=(anywhere, anywhere),
        scratch_shapes=[
            pltpu.VMEM((B, B), f32),
            pltpu.VMEM((STEPS, B, B), f32),
            states,
            states,
            hidden,
            pltpu.VMEM((2, STEPS, 2, B, B), bf16),
            hidden,
            weights,
            weights,
            pltpu.VMEM((CHAINS, 2, Q, B), f32),
            pltpu.VMEM((3 * CHAINS, 3, 2, Q, B), bf16),
            pltpu.VMEM((3 * CHAINS, 2, Q, B), bf16),
            pltpu.VMEM((3 * CHAINS, 2, 2, Q, B), bf16),
            pltpu.VMEM((3 * CHAINS, 4, Q, B), f32),
            pltpu.VMEM((2, 2, B, 4 * B), f32),
            pltpu.VMEM((2, 2, 3, 2, H, B), bf16),
            pltpu.VMEM((2, 2, 2, H, B), bf16),
            pltpu.VMEM((2, 2, 4, H, B), f32),
            pltpu.VMEM((2, 2, 2, 2, H, B), bf16),
            pltpu.VMEM((2, 2, B, B), bf16),
            pltpu.VMEM((2, 4, 8, B), f32),
            pltpu.VMEM((1, B), f32),
            pltpu.VMEM((B, 128), f32),
            pltpu.VMEM((2, 8, B), f32),
            pltpu.VMEM((2, B, 128), f32),
            pltpu.VMEM((2, 4, H, B), bf16),
            pltpu.VMEM((H, 4 * B), bf16),
            pltpu.SMEM((1,), f32),
            pltpu.SemaphoreType.DMA((LEAVING + 8,)),
            pltpu.SemaphoreType.DMA((ARRIVALS + 8,)),
            pltpu.SemaphoreType.DMA((22,)),
        ],
        compiler_params=pltpu.CompilerParams(collective_id=0, has_side_effects=True, vmem_limit_bytes=66000000),
    )(start, increments, w_in.reshape(4, 4, 2, H, B), w_out.reshape(2, H, D), initial.reshape(1))
    return pl.pallas_call(
        placing,
        out_shape=(
            jax.ShapeDtypeStruct((B,), f32),
            jax.ShapeDtypeStruct((2 * B, B), f32),
            jax.ShapeDtypeStruct((B, 2 * B), f32),
        ),
        in_specs=[vmem, vmem],
        out_specs=(vmem, vmem, vmem),
    )(row, blocks)


def solution(mesh):
    finer = Mesh(mesh.devices.reshape(4, 4, 4, 2), ("y", "x", "z", "c"))
    return jax.shard_map(
        on_device,
        mesh=finer,
        in_specs=(P(BATCH, DIM), P(None, BATCH, DIM), P(None, DIM), P(DIM, None), P()),
        out_specs=(P(BATCH), P(BATCH, DIM), P(DIM, BATCH)),
        check_vma=False,
    )
```
